32 devices in a mesh: dp: 2 (over x), row: 4 (over z), col: 4 (over y, core).
Axes of the slice: x: 2, y: 2, z: 4, core: 2. Of those that a mesh axis runs over, the one named last changes fastest.
Arguments:
- x: bfloat16 [256, 4096], P('dp', ('row', 'col')), parts along dimension 0
- ln_gain: bfloat16 [4096], P(('row', 'col'))
- w_in: bfloat16 [4096, 37376], P('row', 'col')
- w_out: bfloat16 [20480, 4096], P('col', 'row')
- k_cache: bfloat16 [256, 2048, 256], P(('dp', 'col', 'row')), parts along dimension 0
- v_cache: bfloat16 [256, 2048, 256], P(('dp', 'col', 'row')), parts along dimension 0
- lengths: int32 [256], P(('dp', 'col', 'row')), parts along dimension 0
- rope_cos: float32 [256, 128], P(('dp', 'col', 'row')), parts along dimension 0
- rope_sin: float32 [256, 128], P(('dp', 'col', 'row')), parts along dimension 0
Outputs:
- output 1: bfloat16 [256, 4096], P('dp', ('row', 'col')), parts along dimension 0
- output 2: bfloat16 [256, 2048, 256], P(('dp', 'col', 'row')), parts along dimension 0
- output 3: bfloat16 [256, 2048, 256], P(('dp', 'col', 'row')), parts along dimension 0
There are 2 independent parts. The reference program is written for one: setup_inputs(seed, part) draws one part's arguments, and reference() takes and returns one part's arrays. A program takes and returns all parts, laid end to end along the dimension named above; an argument that names none is the same for every part.
All inputs are finite; a program needn't handle non-finite values.
Results may differ from the reference program's by a relative error of at most 0.00926775.
Values are sent between devices in bfloat16 or wider.
A program may use at most 1 GiB of HBM per device.

```python
import jax
import jax.numpy as jnp
from jax import lax

D = 4096
HEADS = 16
HEAD = 256
FF_DIM = 16384
SEQS_DEV = 8
CACHE_LEN = 2048
ROW_DEVS = 4
COL_DEVS = 4

NORM_EPS = 1e-6
BATCH_ROWS = SEQS_DEV * ROW_DEVS * COL_DEVS
HALF_HEAD = HEAD // 2
ROW_WIDTH = D // ROW_DEVS
Q_COLS = HEADS * HEAD // COL_DEVS
KV_COLS = HEAD // COL_DEVS
F_COLS = FF_DIM // COL_DEVS
GATE_START = Q_COLS + 2 * KV_COLS
E_COLS = GATE_START + 2 * F_COLS
R_COLS = Q_COLS + F_COLS
N_BLOCKS = ROW_DEVS * COL_DEVS


def draw_lengths(key):
    keys = jax.random.split(key, 3)
    long_len = jax.random.randint(keys[0], (BATCH_ROWS,), 0, CACHE_LEN)
    short_len = jax.random.randint(keys[1], (BATCH_ROWS,), 0, 8)
    pick_short = jax.random.randint(keys[2], (BATCH_ROWS,), 0, 4) == 0
    lengths = jnp.where(pick_short, short_len, long_len).astype(jnp.int32)
    return lengths.at[0].set(CACHE_LEN - 1).at[1].set(0)


def rope_tables(lengths):
    freq_exp = jnp.arange(HALF_HEAD, dtype=jnp.float32) * (2.0 / HEAD)
    inv_freq = jnp.exp(-jnp.log(10000.0) * freq_exp)
    angles = lengths.astype(jnp.float32)[:, None] * inv_freq[None, :]
    return jnp.cos(angles), jnp.sin(angles)


def setup_inputs(seed: int = 0, part: int = 0) -> dict:
    base_key = jax.random.key(seed)
    shared = jax.random.split(base_key, 3)
    own = jax.random.split(jax.random.fold_in(base_key, part), 8)
    ramp = jnp.arange(D, dtype=jnp.float32) / D
    col_scale = (0.5 + 1.5 * ramp) * jnp.exp(0.2 * jax.random.normal(own[0], (D,), jnp.float32))
    col_mean = 1.5 - 2.0 * ramp + 0.3 * jax.random.normal(own[1], (D,), jnp.float32)
    row_mean = 0.5 * jax.random.normal(own[2], (BATCH_ROWS, 1), jnp.float32)
    x = jax.random.normal(own[3], (BATCH_ROWS, D), jnp.float32) * col_scale + col_mean + row_mean
    ln_gain = 1.0 + 0.4 * jax.random.normal(shared[0], (D,), jnp.float32)
    w_in = jax.random.normal(shared[1], (D, COL_DEVS * E_COLS), jnp.float32) * D ** -0.5
    w_out = jax.random.normal(shared[2], (COL_DEVS * R_COLS, D), jnp.float32) * (COL_DEVS * R_COLS) ** -0.5
    seq_mean = 0.8 * jax.random.normal(own[4], (BATCH_ROWS, 1, HEAD), jnp.float32)
    k_cache = 2.0 * jax.random.normal(own[5], (BATCH_ROWS, CACHE_LEN, HEAD), jnp.float32)
    v_cache = jax.random.normal(own[6], (BATCH_ROWS, CACHE_LEN, HEAD), jnp.float32) + seq_mean
    lengths = draw_lengths(own[7])
    rope_cos, rope_sin = rope_tables(lengths)
    return {'x': x.astype(jnp.bfloat16), 'ln_gain': ln_gain.astype(jnp.bfloat16), 'w_in': w_in.astype(jnp.bfloat16), 'w_out': w_out.astype(jnp.bfloat16), 'k_cache': k_cache.astype(jnp.bfloat16), 'v_cache': v_cache.astype(jnp.bfloat16), 'lengths': lengths, 'rope_cos': rope_cos, 'rope_sin': rope_sin}


def apply_rope(vals, cos_t, sin_t):
    first = vals[..., :HALF_HEAD]
    second = vals[..., HALF_HEAD:]
    return jnp.concatenate([first * cos_t - second * sin_t, second * cos_t + first * sin_t], axis=-1)


def block_sum(acc, pair):
    part_sum = jnp.dot(pair[0], pair[1], preferred_element_type=jnp.float32)
    return acc + part_sum.astype(jnp.bfloat16).astype(jnp.float32), None


def attend(block):
    queries, k_blk, v_blk, len_blk = block
    scores = jnp.einsum('bhd,btd->bht', queries.astype(jnp.float32), k_blk.astype(jnp.float32))
    visible = jnp.arange(CACHE_LEN)[None, None, :] <= len_blk[:, None, None]
    attn_probs = jax.nn.softmax(jnp.where(visible, scores, -1e30), axis=-1).astype(jnp.bfloat16)
    return jnp.einsum('bht,btd->bhd', attn_probs.astype(jnp.float32), v_blk.astype(jnp.float32)).astype(jnp.bfloat16)


def reference(x, ln_gain, w_in, w_out, k_cache, v_cache, lengths, rope_cos, rope_sin):
    x_float = x.astype(jnp.float32)
    mean = jnp.mean(x_float, axis=1, keepdims=True)
    variance = jnp.mean(jnp.square(x_float - mean), axis=1, keepdims=True)
    normed = ((x_float - mean) * lax.rsqrt(variance + NORM_EPS) * ln_gain.astype(jnp.float32)).astype(jnp.bfloat16)
    h_blocks = normed.reshape(BATCH_ROWS, ROW_DEVS, ROW_WIDTH).transpose(1, 0, 2)
    w_blocks = w_in.reshape(ROW_DEVS, ROW_WIDTH, COL_DEVS * E_COLS)
    in_sum, _ = lax.scan(block_sum, jnp.zeros((BATCH_ROWS, COL_DEVS * E_COLS), jnp.float32), (h_blocks, w_blocks))
    projected = in_sum.astype(jnp.bfloat16).reshape(BATCH_ROWS, COL_DEVS, E_COLS)
    q_raw = projected[:, :, :Q_COLS].reshape(BATCH_ROWS, HEADS, HEAD).astype(jnp.float32)
    k_raw = projected[:, :, Q_COLS:Q_COLS + KV_COLS].reshape(BATCH_ROWS, HEAD).astype(jnp.float32)
    v_new = projected[:, :, Q_COLS + KV_COLS:GATE_START].reshape(BATCH_ROWS, HEAD)
    gate_in = projected[:, :, GATE_START:GATE_START + F_COLS].astype(jnp.float32)
    up_in = projected[:, :, GATE_START + F_COLS:].astype(jnp.float32)
    mixed = (jax.nn.silu(gate_in) * up_in).astype(jnp.bfloat16)
    queries = (apply_rope(q_raw, rope_cos[:, None, :], rope_sin[:, None, :]) * HEAD ** -0.5).astype(jnp.bfloat16)
    k_new = apply_rope(k_raw, rope_cos, rope_sin).astype(jnp.bfloat16)
    new_slot = (jnp.arange(CACHE_LEN)[None, :] == lengths[:, None])[:, :, None]
    k_out = jnp.where(new_slot, k_new[:, None, :], k_cache)
    v_out = jnp.where(new_slot, v_new[:, None, :], v_cache)
    attn_out = lax.map(attend, (queries.reshape(N_BLOCKS, SEQS_DEV, HEADS, HEAD), k_out.reshape(N_BLOCKS, SEQS_DEV, CACHE_LEN, HEAD), v_out.reshape(N_BLOCKS, SEQS_DEV, CACHE_LEN, HEAD), lengths.reshape(N_BLOCKS, SEQS_DEV)))
    out_inputs = jnp.concatenate([attn_out.reshape(BATCH_ROWS, COL_DEVS, Q_COLS), mixed], axis=2).transpose(1, 0, 2)
    w_out_blocks = w_out.reshape(COL_DEVS, R_COLS, D)
    out_sum, _ = lax.scan(block_sum, jnp.zeros((BATCH_ROWS, D), jnp.float32), (out_inputs, w_out_blocks))
    delta = out_sum.astype(jnp.bfloat16).astype(jnp.float32)
    y = (x_float + delta).astype(jnp.bfloat16)
    return (y, k_out, v_out)
```

```python
import functools

import jax
import jax.numpy as jnp
from jax import lax
from jax.experimental import pallas as pl
from jax.experimental.pallas import tpu as pltpu
from jax.sharding import PartitionSpec as P

NORM_EPS = 1e-6
MESH = pl.DeviceIdType.MESH
F32 = jnp.float32
BF16 = jnp.bfloat16
CHUNK = 128
LEAD = 3
GAIN_ROWS = 16


def layer_kernel(dims, xs_ref, win_ref, wout_ref, kc_ref, vc_ref, len_ref, cos_ref, sin_ref,
                 y_ref, knew_ref, vnew_ref,
                 wq, wgu, wo, kbuf, vbuf, xg, st, h, part, rbuf, mful, qsend, qrecv, qhm, qsm, kn3, vn3, osm,
                 asend, arecv, acc, ysend, yrecv,
                 wsem, kvsem, xs_s, xs_r, st_s, st_r, q_s, q_r, rs_s, rs_r, ag_s, ag_r, at_s, at_r, y_s, y_r):
    rows, cols, n_chunks, w, q_cols, kv_cols, f_cols = dims
    group = rows * cols
    dp, r, c = lax.axis_index("dp"), lax.axis_index("row"), lax.axis_index("col")
    me = c * rows + r
    batch, xw = y_ref.shape
    seqs = batch // group
    gate_start = q_cols + 2 * kv_cols
    half_f = f_cols // 2
    heads_c = q_cols // 256
    heads = heads_c * cols
    cache_len = kbuf.shape[1]

    def dev(g):
        return (dp, g % rows, g // rows)

    def wq_copy():
        return pltpu.make_async_copy(win_ref.at[:, pl.ds(0, gate_start)], wq, wsem.at[4 * n_chunks])

    def wgu_copy(d, k, part_id):
        col = gate_start + part_id * f_cols + d * half_f + k * w
        return pltpu.make_async_copy(win_ref.at[:, pl.ds(pl.multiple_of(col, 128), w)],
                                     wgu.at[d, k, :, pl.ds(part_id * w, w)],
                                     wsem.at[(d * n_chunks + k) * 2 + part_id])

    def kv_copy(b, which):
        src, dst = ((kc_ref, kbuf), (vc_ref, vbuf))[which]
        return pltpu.make_async_copy(src.at[b], dst.at[b], kvsem.at[which, b])

    def wo_copy():
        return pltpu.make_async_copy(wout_ref, wo, wsem.at[4 * n_chunks + 1])

    wq_copy().start()

    @pl.loop(0, n_chunks)
    def _(k):
        for d in range(2):
            for s in range(2):
                wgu_copy(d, k, s).start()

    @pl.loop(0, seqs)
    def _(b):
        kv_copy(b, 0).start()
        kv_copy(b, 1).start()

    wo_copy().start()

    barrier = pltpu.get_barrier_semaphore()

    @pl.loop(1, group)
    def _(j):
        pl.semaphore_signal(barrier, inc=1, device_id=dev((me + j) % group), device_id_type=MESH)

    x_own = xs_ref[0:batch, :].astype(F32)
    s_own = jnp.sum(x_own, axis=1, keepdims=True)
    m2_own = jnp.sum(jnp.square(x_own - s_own * (1.0 / xw)), axis=1, keepdims=True)
    lane = lax.broadcasted_iota(jnp.int32, (batch, 128), 1)
    table = jnp.where(lane == 0, s_own, jnp.where(lane == 1, m2_own, 0.0))
    st[me] = table.T[0:8, :]

    pl.semaphore_wait(barrier, group - 1)

    def st_copy(slot, peer):
        return pltpu.make_async_remote_copy(st.at[slot], st.at[slot], st_s.at[peer], st_r.at[slot],
                                            device_id=dev(peer), device_id_type=MESH)

    def x_copy(slot, peer_c):
        return pltpu.make_async_remote_copy(xs_ref, xg.at[slot], xs_s.at[peer_c], xs_r.at[slot],
                                            device_id=(dp, r, peer_c), device_id_type=MESH)

    @pl.loop(1, group)
    def _(j):
        st_copy(me, (me + j) % group).start()

    @pl.loop(1, cols)
    def _(j):
        x_copy(c, (c + j) % cols).start()

    xg[c] = xs_ref[...]

    @pl.loop(1, group)
    def _(j):
        src = (me + j) % group
        st_copy(src, src).wait_recv()

    stats = st[...]
    sums = stats[:, 0:1, :]
    width = xw * group
    mean_row = jnp.sum(sums, axis=0) * (1.0 / width)
    dev_mean = sums * (1.0 / xw) - mean_row[None]
    m2_row = jnp.sum(stats[:, 1:2, :] + xw * jnp.square(dev_mean), axis=0)
    inv_row = lax.rsqrt(m2_row * (1.0 / width) + NORM_EPS)
    sub = lax.broadcasted_iota(jnp.int32, (128, batch), 0)
    back = jnp.where(sub == 0, mean_row, jnp.where(sub == 1, inv_row, 0.0)).T
    mean = back[:, 0:1]
    inv = back[:, 1:2]

    @pl.loop(1, cols)
    def _(j):
        src = (c + j) % cols
        x_copy(src, src).wait_recv()

    for cc in range(cols):
        xv = xg[cc, 0:batch, :].astype(F32)
        gain = xg[cc, batch:batch + GAIN_ROWS, :].astype(F32)[0:1, :]
        h[:, cc * xw:(cc + 1) * xw] = ((xv - mean) * inv * gain).astype(BF16)

    def q_copy(slot, peer):
        return pltpu.make_async_remote_copy(qsend.at[peer], qrecv.at[slot], q_s.at[peer], q_r.at[slot],
                                            device_id=dev(peer), device_id_type=MESH)

    wq_copy().wait()
    qkv = jnp.dot(h[...], wq[...], preferred_element_type=F32)
    qsend[...] = qkv.reshape(group, seqs, gate_start).astype(BF16)
    qrecv[me] = qsend[me]

    @pl.loop(1, group)
    def _(j):
        q_copy(me, (me + j) % group).start()

    acc[...] = jnp.zeros_like(acc)

    def rs_copy(d, k):
        nxt = (dp, r + 1, c) if d == 0 else (dp, r - 1, c)
        return pltpu.make_async_remote_copy(part.at[d, k], rbuf.at[d, k], rs_s.at[d, k], rs_r.at[d, k],
                                            device_id=nxt, device_id_type=MESH)

    def ag_copy(d, k):
        nxt = (dp, r - 1, c) if d == 0 else (dp, r + 1, c)
        return pltpu.make_async_remote_copy(mful.at[d, k], mful.at[d, k], ag_s.at[d, k], ag_r.at[d, k],
                                            device_id=nxt, device_id_type=MESH)

    pos = (r, rows - 1 - r)

    def partial_step(k):
        for d in range(2):
            wgu_copy(d, k, 0).wait()
            wgu_copy(d, k, 1).wait()
            part[d, k] = jnp.dot(h[...], wgu[d, k], preferred_element_type=F32).astype(BF16)

            @pl.when(pos[d] == 0)
            def _():
                rs_copy(d, k).start()

    def out_step(d, k):
        row0 = pl.multiple_of(q_cols + d * half_f + k * w, 128)
        acc[...] += jnp.dot(mful[d, k], wo[pl.ds(row0, w), :], preferred_element_type=F32)

    def reduce_step(d, k):
        total = part[d, k].astype(F32) + rbuf[d, k].astype(F32)

        @pl.when(pos[d] < rows - 1)
        def _():
            part[d, k] = total.astype(BF16)
            rs_copy(d, k).start()

        @pl.when(pos[d] == rows - 1)
        def _():
            full = total.astype(BF16).astype(F32)
            gate, up = full[:, :w], full[:, w:]
            mful[d, k] = (jax.nn.silu(gate) * up).astype(BF16)
            ag_copy(d, k).start()
            out_step(d, k)

    def prepare_queries():
        @pl.loop(1, group)
        def _(j):
            src = (me + j) % group
            q_copy(src, src).wait_recv()

        cos_t, sin_t = cos_ref[...], sin_ref[...]

        def rope(v):
            first, second = v[:, :128], v[:, 128:]
            return jnp.concatenate([first * cos_t - second * sin_t, second * cos_t + first * sin_t], axis=-1)

        k_parts, v_parts = [], []
        for cc in range(cols):
            full = qrecv[cc * rows].astype(F32)
            for rr in range(1, rows):
                full = full + qrecv[cc * rows + rr].astype(F32)
            full = full.astype(BF16).astype(F32)
            for i in range(heads_c):
                qhm[cc * heads_c + i] = rope(full[:, i * 256:(i + 1) * 256]) * (256 ** -0.5)
            k_parts.append(full[:, q_cols:q_cols + kv_cols])
            v_parts.append(full[:, q_cols + kv_cols:gate_start])
        k_row = rope(jnp.concatenate(k_parts, axis=-1)).astype(BF16)
        v_row = jnp.concatenate(v_parts, axis=-1).astype(BF16)
        knew_ref[...] = k_row
        vnew_ref[...] = v_row
        k_row, v_row = k_row.astype(F32), v_row.astype(F32)
        for b in range(seqs):
            qsm[b] = qhm[:, b, :].astype(BF16)
            kn3[b] = jnp.broadcast_to(k_row[b:b + 1, :], (8, 256))
            vn3[b] = jnp.broadcast_to(v_row[b:b + 1, :], (8, 256))

    def attend(b):
        kv_copy(b, 0).wait()
        kv_copy(b, 1).wait()
        q = qsm[b]
        limit = len_ref[b][0:1, 0:1]
        where_t = lax.broadcasted_iota(jnp.int32, (heads, cache_len), 1)
        scores = lax.dot_general(q, kbuf[b], (((1,), (1,)), ((), ())), preferred_element_type=F32)
        s_new = jnp.sum(q.astype(F32) * kn3[b][0:1, :], axis=1, keepdims=True)
        scores = jnp.where(where_t == limit, s_new, scores)
        scores = jnp.where(where_t <= limit, scores, -1e30)
        e = jnp.exp(scores - jnp.max(scores, axis=1, keepdims=True))
        probs = (e / jnp.sum(e, axis=1, keepdims=True)).astype(BF16).astype(F32)
        p_new = jnp.sum(jnp.where(where_t == limit, probs, 0.0), axis=1, keepdims=True)
        p_old = jnp.where(where_t == limit, 0.0, probs).astype(BF16)
        osm[b] = jnp.dot(p_old, vbuf[b], preferred_element_type=F32) + p_new * vn3[b][0:1, :]

    def at_copy(slot, peer):
        return pltpu.make_async_remote_copy(asend.at[peer // rows], arecv.at[slot], at_s.at[peer], at_r.at[slot],
                                            device_id=dev(peer), device_id_type=MESH)

    def send_attention():
        for cc in range(cols):
            asend[cc] = jnp.concatenate([osm[:, cc * heads_c + i, :] for i in range(heads_c)], axis=-1).astype(BF16)
        arecv[me] = asend[c]

        @pl.loop(1, group)
        def _(j):
            at_copy(me, (me + j) % group).start()

    @pl.loop(0, LEAD)
    def _(k):
        partial_step(k)

    first_attn = 3

    @pl.loop(0, n_chunks + 10)
    def _(i):
        @pl.when(i + LEAD < n_chunks)
        def _():
            partial_step(i + LEAD)

        for d in range(2):
            p = pos[d]
            k = i - (p + p // 2)

            @pl.when((p > 0) & (k >= 0) & (k < n_chunks))
            def _():
                rs_copy(d, k).wait_recv()
                reduce_step(d, k)

        for d in range(2):
            q = rows - 1 - pos[d]
            k = i - (5 + q + q // 2)

            @pl.when((q > 0) & (k >= 0) & (k < n_chunks))
            def _():
                ag_copy(d, k).wait_recv()

                @pl.when(q < rows - 1)
                def _():
                    ag_copy(d, k).start()

                out_step(d, k)

        @pl.when(i == first_attn - 1)
        def _():
            wo_copy().wait()
            prepare_queries()

        @pl.when((i >= first_attn) & (i < first_attn + seqs))
        def _():
            attend(i - first_attn)

        @pl.when(i == first_attn + seqs)
        def _():
            send_attention()

    @pl.loop(1, group)
    def _(j):
        src = (me + j) % group
        at_copy(src, src).wait_recv()

    attn = arecv[...].astype(F32).reshape(batch, q_cols).astype(BF16)
    total = (acc[...] + jnp.dot(attn, wo[0:q_cols, :], preferred_element_type=F32)).astype(BF16)
    for cc in range(cols):
        ysend[cc] = total[:, cc * xw:(cc + 1) * xw]

    def y_copy(slot, peer_c):
        return pltpu.make_async_remote_copy(ysend.at[peer_c], yrecv.at[slot], y_s.at[peer_c], y_r.at[slot],
                                            device_id=(dp, r, peer_c), device_id_type=MESH)

    @pl.loop(1, cols)
    def _(j):
        y_copy(c, (c + j) % cols).start()

    yrecv[c] = ysend[c]

    @pl.loop(1, group)
    def _(j):
        peer = (me + j) % group
        st_copy(me, peer).wait_send()
        q_copy(me, peer).wait_send()
        at_copy(me, peer).wait_send()

    @pl.loop(1, cols)
    def _(j):
        x_copy(c, (c + j) % cols).wait_send()

    @pl.loop(0, n_chunks)
    def _(k):
        for d in range(2):
            @pl.when(pos[d] < rows - 1)
            def _():
                rs_copy(d, k).wait_send()

            @pl.when(pos[d] > 0)
            def _():
                ag_copy(d, k).wait_send()

    @pl.loop(1, cols)
    def _(j):
        src = (c + j) % cols
        y_copy(src, src).wait_recv()

    delta = yrecv[0].astype(F32)
    for cc in range(1, cols):
        delta = delta + yrecv[cc].astype(F32)
    y_ref[...] = (xs_ref[0:batch, :].astype(F32) + delta.astype(BF16).astype(F32)).astype(BF16)

    @pl.loop(1, cols)
    def _(j):
        y_copy(c, (c + j) % cols).wait_send()


def solution(mesh):
    rows = mesh.shape['row']
    cols = mesh.shape['col']
    seq_spec = P(('dp', 'col', 'row'))
    act_spec = P('dp', ('row', 'col'))

    def local_layer(x, ln_gain, w_in, w_out, k_cache, v_cache, lengths, rope_cos, rope_sin):
        batch, xw = x.shape
        group = rows * cols
        seqs = batch // group
        head = rope_cos.shape[1] * 2
        cache_len = k_cache.shape[1]
        kdim, e_cols = w_in.shape
        r_cols, n_out = w_out.shape
        kv_cols = head // cols
        f_cols = e_cols - r_cols - 2 * kv_cols
        q_cols = r_cols - f_cols
        gate_start = q_cols + 2 * kv_cols
        heads = q_cols * cols // head
        w = CHUNK
        n_chunks = f_cols // 2 // w
        dims = (rows, cols, n_chunks, w, q_cols, kv_cols, f_cols)
        xs = jnp.concatenate([x, jnp.broadcast_to(ln_gain[None, :], (GAIN_ROWS, xw))], axis=0)
        len3 = jnp.broadcast_to(lengths[:, None, None], (seqs, 8, 128))
        vmem = pl.BlockSpec(memory_space=pltpu.VMEM)
        hbm = pl.BlockSpec(memory_space=pl.ANY)
        dma = pltpu.SemaphoreType.DMA
        y, k_new, v_new = pl.pallas_call(
            functools.partial(layer_kernel, dims),
            out_shape=(jax.ShapeDtypeStruct((batch, xw), BF16), jax.ShapeDtypeStruct((seqs, head), BF16),
                       jax.ShapeDtypeStruct((seqs, head), BF16)),
            in_specs=[vmem, hbm, hbm, hbm, hbm, vmem, vmem, vmem],
            out_specs=(vmem, vmem, vmem),
            scratch_shapes=[
                pltpu.VMEM((kdim, gate_start), BF16),
                pltpu.VMEM((2, n_chunks, kdim, 2 * w), BF16),
                pltpu.VMEM((r_cols, n_out), BF16),
                pltpu.VMEM((seqs, cache_len, head), BF16),
                pltpu.VMEM((seqs, cache_len, head), BF16),
                pltpu.VMEM((cols, batch + GAIN_ROWS, xw), BF16),
                pltpu.VMEM((group, 8, batch), F32),
                pltpu.VMEM((batch, kdim), BF16),
                pltpu.VMEM((2, n_chunks, batch, 2 * w), BF16),
                pltpu.VMEM((2, n_chunks, batch, 2 * w), BF16),
                pltpu.VMEM((2, n_chunks, batch, w), BF16),
                pltpu.VMEM((group, seqs, gate_start), BF16),
                pltpu.VMEM((group, seqs, gate_start), BF16),
                pltpu.VMEM((heads, seqs, head), F32),
                pltpu.VMEM((seqs, heads, head), BF16),
                pltpu.VMEM((seqs, 8, head), F32),
                pltpu.VMEM((seqs, 8, head), F32),
                pltpu.VMEM((seqs, heads, head), F32),
                pltpu.VMEM((cols, seqs, q_cols), BF16),
                pltpu.VMEM((group, seqs, q_cols), BF16),
                pltpu.VMEM((batch, n_out), F32),
                pltpu.VMEM((cols, batch, xw), BF16),
                pltpu.VMEM((cols, batch, xw), BF16),
                dma((4 * n_chunks + 2,)), dma((2, seqs)),
                dma((cols,)), dma((cols,)), dma((group,)), dma((group,)), dma((group,)), dma((group,)),
                dma((2, n_chunks)), dma((2, n_chunks)), dma((2, n_chunks)), dma((2, n_chunks)),
                dma((group,)), dma((group,)), dma((cols,)), dma((cols,)),
            ],
            compiler_params=pltpu.CompilerParams(collective_id=0, has_side_effects=True,
                                                 vmem_limit_bytes=62 * 1024 * 1024),
            name="layer",
        )(xs, w_in, w_out, k_cache, v_cache, len3, rope_cos, rope_sin)
        new_slot = (jnp.arange(cache_len)[None, :] == lengths[:, None])[:, :, None]
        k_out = jnp.where(new_slot, k_new[:, None, :], k_cache)
        v_out = jnp.where(new_slot, v_new[:, None, :], v_cache)
        return y, k_out, v_out

    return jax.shard_map(local_layer, mesh=mesh, in_specs=(act_spec, P(('row', 'col')), P('row', 'col'), P('col', 'row'), seq_spec, seq_spec, seq_spec, seq_spec, seq_spec), out_specs=(act_spec, seq_spec, seq_spec), check_vma=False)
```

```python
import contextlib
import functools

import jax
import jax.numpy as jnp
from jax import lax
from jax.experimental import pallas as pl
from jax.experimental.pallas import tpu as pltpu
from jax.sharding import PartitionSpec as P

NORM_EPS = 1e-6
MESH = pl.DeviceIdType.MESH
F32 = jnp.float32
BF16 = jnp.bfloat16
CHUNK = 128
ATTN_AT = 2
SEND_AT = 10
GATHER_AT = 15
PROFILE = False


def scope(name):
    return jax.named_scope(name) if PROFILE else contextlib.nullcontext()


def layer_kernel(dims, len_ref, x_ref, gain_ref, win_ref, wout_ref, kc_ref, vc_ref, cos_ref, sin_ref,
                 y_ref, kbuf, vbuf,
                 wq, wgu, wo, xg, gg, st, h, part, rbuf, mful, qsend, qrecv, qhm, qsm, kn3, vn3, osm,
                 asend, arecv, acc, ysend, yrecv,
                 wsem, kvsem, xs_s, xs_r, g_s, g_r, st_s, st_r, q_s, q_r, rs_s, rs_r, ag_s, ag_r, at_s, at_r, y_s, y_r):
    rows, cols, n_chunks, w, q_cols, kv_cols, f_cols = dims
    group = rows * cols
    dp, r, c = lax.axis_index("dp"), lax.axis_index("row"), lax.axis_index("col")
    me = c * rows + r
    batch, xw = y_ref.shape
    seqs = batch // group
    gate_start = q_cols + 2 * kv_cols
    half_f = f_cols // 2
    heads_c = q_cols // 256
    heads = heads_c * cols
    cache_len, head = kbuf.shape[1:]

    def dev(g):
        return (dp, g % rows, g // rows)

    def wq_copy():
        return pltpu.make_async_copy(win_ref.at[:, pl.ds(0, gate_start)], wq, wsem.at[4 * n_chunks])

    def wgu_copy(d, k, part_id):
        col = gate_start + part_id * f_cols + d * half_f + k * w
        return pltpu.make_async_copy(win_ref.at[:, pl.ds(pl.multiple_of(col, 128), w)],
                                     wgu.at[k, :, pl.ds((2 * d + part_id) * w, w)],
                                     wsem.at[(d * n_chunks + k) * 2 + part_id])

    def kv_copy(b, which):
        src, dst = ((kc_ref, kbuf), (vc_ref, vbuf))[which]
        return pltpu.make_async_copy(src.at[b], dst.at[b], kvsem.at[which, b])

    def wo_copy():
        return pltpu.make_async_copy(wout_ref, wo, wsem.at[4 * n_chunks + 1])

    wq_copy().start()

    @pl.loop(0, n_chunks)
    def _(k):
        for d in range(2):
            for s in range(2):
                wgu_copy(d, k, s).start()

    @pl.loop(0, seqs)
    def _(b):
        kv_copy(b, 0).start()
        kv_copy(b, 1).start()

    wo_copy().start()

    barrier = pltpu.get_barrier_semaphore()

    @pl.loop(1, group)
    def _(j):
        pl.semaphore_signal(barrier, inc=1, device_id=dev((me + j) % group), device_id_type=MESH)

    x_own = x_ref[...].astype(F32)
    s_own = jnp.sum(x_own, axis=1, keepdims=True)
    m2_own = jnp.sum(jnp.square(x_own - s_own * (1.0 / xw)), axis=1, keepdims=True)
    lane = lax.broadcasted_iota(jnp.int32, (batch, 128), 1)
    table = jnp.where(lane == 0, s_own, jnp.where(lane == 1, m2_own, 0.0))
    st[me] = table.T[0:8, :]
    gg[c] = jnp.broadcast_to(gain_ref[...].astype(F32), (8, xw))

    with scope('barrier'):
        pl.semaphore_wait(barrier, group - 1)

    def st_copy(slot, peer):
        return pltpu.make_async_remote_copy(st.at[slot], st.at[slot], st_s.at[peer], st_r.at[slot],
                                            device_id=dev(peer), device_id_type=MESH)

    def x_copy(slot, peer_c):
        return pltpu.make_async_remote_copy(x_ref, xg.at[slot], xs_s.at[peer_c], xs_r.at[slot],
                                            device_id=(dp, r, peer_c), device_id_type=MESH)

    def g_copy(slot, peer_c):
        return pltpu.make_async_remote_copy(gg.at[slot], gg.at[slot], g_s.at[peer_c], g_r.at[slot],
                                            device_id=(dp, r, peer_c), device_id_type=MESH)

    @pl.loop(1, group)
    def _(j):
        st_copy(me, (me + j) % group).start()

    @pl.loop(1, cols)
    def _(j):
        x_copy(c, (c + j) % cols).start()
        g_copy(c, (c + j) % cols).start()

    xg[c] = x_ref[...]

    @pl.loop(1, group)
    def _(j):
        src = (me + j) % group
        with scope('stats'):
            st_copy(src, src).wait_recv()

    stats = st[...]
    sums = stats[:, 0:1, :]
    width = xw * group
    mean_row = jnp.sum(sums, axis=0) * (1.0 / width)
    dev_mean = sums * (1.0 / xw) - mean_row[None]
    m2_row = jnp.sum(stats[:, 1:2, :] + xw * jnp.square(dev_mean), axis=0)
    inv_row = lax.rsqrt(m2_row * (1.0 / width) + NORM_EPS)
    sub = lax.broadcasted_iota(jnp.int32, (128, batch), 0)
    back = jnp.where(sub == 0, mean_row, jnp.where(sub == 1, inv_row, 0.0)).T
    mean = back[:, 0:1]
    inv = back[:, 1:2]

    @pl.loop(1, cols)
    def _(j):
        src = (c + j) % cols
        with scope('xwait'):
            x_copy(src, src).wait_recv()
            g_copy(src, src).wait_recv()

    for cc in range(cols):
        xv = xg[cc].astype(F32)
        gain = gg[cc, 0:1, :]
        h[:, cc * xw:(cc + 1) * xw] = ((xv - mean) * inv * gain).astype(BF16)

    def q_copy(slot, peer):
        return pltpu.make_async_remote_copy(qsend.at[peer], qrecv.at[slot], q_s.at[peer], q_r.at[slot],
                                            device_id=dev(peer), device_id_type=MESH)

    with scope('wqwait'):
        wq_copy().wait()
    qkv = jnp.dot(h[...], wq[...], preferred_element_type=F32)
    qsend[...] = qkv.reshape(group, seqs, gate_start).astype(BF16)
    qrecv[me] = qsend[me]

    @pl.loop(1, group)
    def _(j):
        q_copy(me, (me + j) % group).start()

    acc[...] = jnp.zeros_like(acc)

    def rs_copy(d, k):
        nxt = (dp, r + 1, c) if d == 0 else (dp, r - 1, c)
        return pltpu.make_async_remote_copy(part.at[d, k], rbuf.at[d, k], rs_s.at[d, k], rs_r.at[d, k],
                                            device_id=nxt, device_id_type=MESH)

    def ag_copy(d, k):
        nxt = (dp, r - 1, c) if d == 0 else (dp, r + 1, c)
        return pltpu.make_async_remote_copy(mful.at[d, k], mful.at[d, k], ag_s.at[d, k], ag_r.at[d, k],
                                            device_id=nxt, device_id_type=MESH)

    pos = (r, rows - 1 - r)

    def partial_step(k):
        for d in range(2):
            wgu_copy(d, k, 0).wait()
            wgu_copy(d, k, 1).wait()
        both = jnp.dot(h[...], wgu[k], preferred_element_type=F32).astype(BF16)
        for d in range(2):
            part[d, k] = both[:, d * 2 * w:(d + 1) * 2 * w]

            @pl.when(pos[d] == 0)
            def _():
                rs_copy(d, k).start()

    def out_step(d, k):
        row0 = pl.multiple_of(q_cols + d * half_f + k * w, 128)
        acc[...] += jnp.dot(mful[d, k], wo[pl.ds(row0, w), :], preferred_element_type=F32)

    def reduce_step(d, k):
        total = part[d, k].astype(F32) + rbuf[d, k].astype(F32)

        @pl.when(pos[d] < rows - 1)
        def _():
            part[d, k] = total.astype(BF16)
            rs_copy(d, k).start()

        @pl.when(pos[d] == rows - 1)
        def _():
            full = total.astype(BF16).astype(F32)
            gate, up = full[:, :w], full[:, w:]
            mful[d, k] = (jax.nn.silu(gate) * up).astype(BF16)
            ag_copy(d, k).start()
            out_step(d, k)

    def prepare_queries():
        @pl.loop(1, group)
        def _(j):
            src = (me + j) % group
            q_copy(src, src).wait_recv()

        cos_t, sin_t = cos_ref[...], sin_ref[...]

        def rope(v):
            first, second = v[:, :128], v[:, 128:]
            return jnp.concatenate([first * cos_t - second * sin_t, second * cos_t + first * sin_t], axis=-1)

        k_parts, v_parts = [], []
        for cc in range(cols):
            full = qrecv[cc * rows].astype(F32)
            for rr in range(1, rows):
                full = full + qrecv[cc * rows + rr].astype(F32)
            full = full.astype(BF16).astype(F32)
            for i in range(heads_c):
                qhm[cc * heads_c + i] = rope(full[:, i * 256:(i + 1) * 256]) * (256 ** -0.5)
            k_parts.append(full[:, q_cols:q_cols + kv_cols])
            v_parts.append(full[:, q_cols + kv_cols:gate_start])
        k_row = rope(jnp.concatenate(k_parts, axis=-1)).astype(BF16)
        v_row = jnp.concatenate(v_parts, axis=-1).astype(BF16)
        k_row, v_row = k_row.astype(F32), v_row.astype(F32)
        for b in range(seqs):
            qsm[b] = qhm[:, b, :].astype(BF16)
            kn3[b] = jnp.broadcast_to(k_row[b:b + 1, :], (8, 256))
            vn3[b] = jnp.broadcast_to(v_row[b:b + 1, :], (8, 256))

    def attend(b):
        kv_copy(b, 0).wait()
        kv_copy(b, 1).wait()
        limit = len_ref[b]
        slot = lax.broadcasted_iota(jnp.int32, (cache_len, head), 0) == limit
        k_all = jnp.where(slot, kn3[b][0:1, :].astype(BF16), kbuf[b])
        v_all = jnp.where(slot, vn3[b][0:1, :].astype(BF16), vbuf[b])
        kbuf[b] = k_all
        vbuf[b] = v_all
        scores = lax.dot_general(qsm[b], k_all, (((1,), (1,)), ((), ())), preferred_element_type=F32)
        where_t = lax.broadcasted_iota(jnp.int32, (heads, cache_len), 1)
        scores = jnp.where(where_t <= limit, scores, -1e30)
        e = jnp.exp(scores - jnp.max(scores, axis=1, keepdims=True))
        probs = (e / jnp.sum(e, axis=1, keepdims=True)).astype(BF16)
        osm[b] = jnp.dot(probs, v_all, preferred_element_type=F32)

    def at_copy(slot, peer):
        return pltpu.make_async_remote_copy(asend.at[peer // rows], arecv.at[slot], at_s.at[peer], at_r.at[slot],
                                            device_id=dev(peer), device_id_type=MESH)

    def send_attention():
        for cc in range(cols):
            asend[cc] = jnp.concatenate([osm[:, cc * heads_c + i, :] for i in range(heads_c)], axis=-1).astype(BF16)
        arecv[me] = asend[c]

        @pl.loop(1, group)
        def _(j):
            at_copy(me, (me + j) % group).start()

    @pl.loop(0, n_chunks)
    def _(k):
        with scope('partial'):
            partial_step(k)

    @pl.loop(0, GATHER_AT + 2 * (rows - 2) + n_chunks // 2)
    def _(i):
        for d in range(2):
            p = pos[d]
            k = i - 2 * (p - 1)

            @pl.when((p > 0) & (k >= 0) & (k < n_chunks))
            def _():
                with scope('rswait%d' % d):
                    rs_copy(d, k).wait_recv()
                with scope('reduce%d' % d):
                    reduce_step(d, k)

        for d in range(2):
            q = rows - 1 - pos[d]
            k2 = i - GATHER_AT - 2 * (q - 1)

            @pl.when((q > 0) & (k2 >= 0) & (k2 < n_chunks // 2))
            def _():
                for k in (2 * k2, 2 * k2 + 1):
                    with scope('agwait%d' % d):
                        ag_copy(d, k).wait_recv()

                    @pl.when(q < rows - 1)
                    def _():
                        ag_copy(d, k).start()

                    with scope('outstep'):
                        out_step(d, k)

        @pl.when(i == ATTN_AT - 1)
        def _():
            with scope('prepare'):
                wo_copy().wait()
                prepare_queries()

        @pl.when((i >= ATTN_AT) & (i < ATTN_AT + seqs))
        def _():
            with scope('attend'):
                attend(i - ATTN_AT)

        @pl.when(i == SEND_AT)
        def _():
            with scope('sendattn'):
                send_attention()

    @pl.loop(1, group)
    def _(j):
        src = (me + j) % group
        with scope('atwait'):
            at_copy(src, src).wait_recv()

    with scope('final'):
        attn = arecv[...].astype(F32).reshape(batch, q_cols).astype(BF16)
        total = (acc[...] + jnp.dot(attn, wo[0:q_cols, :], preferred_element_type=F32)).astype(BF16)
        for cc in range(cols):
            ysend[cc] = total[:, cc * xw:(cc + 1) * xw]

    def y_copy(slot, peer_c):
        return pltpu.make_async_remote_copy(ysend.at[peer_c], yrecv.at[slot], y_s.at[peer_c], y_r.at[slot],
                                            device_id=(dp, r, peer_c), device_id_type=MESH)

    @pl.loop(1, cols)
    def _(j):
        y_copy(c, (c + j) % cols).start()

    yrecv[c] = ysend[c]

    @pl.loop(1, group)
    def _(j):
        peer = (me + j) % group
        st_copy(me, peer).wait_send()
        q_copy(me, peer).wait_send()
        at_copy(me, peer).wait_send()

    @pl.loop(1, cols)
    def _(j):
        x_copy(c, (c + j) % cols).wait_send()
        g_copy(c, (c + j) % cols).wait_send()

    @pl.loop(0, n_chunks)
    def _(k):
        for d in range(2):
            @pl.when(pos[d] < rows - 1)
            def _():
                rs_copy(d, k).wait_send()

            @pl.when(pos[d] > 0)
            def _():
                ag_copy(d, k).wait_send()

    @pl.loop(1, cols)
    def _(j):
        src = (c + j) % cols
        with scope('ywait'):
            y_copy(src, src).wait_recv()

    with scope('yout'):
        delta = yrecv[0].astype(F32)
        for cc in range(1, cols):
            delta = delta + yrecv[cc].astype(F32)
        y_ref[...] = (x_ref[...].astype(F32) + delta.astype(BF16).astype(F32)).astype(BF16)

    @pl.loop(1, cols)
    def _(j):
        with scope('ysent'):
            y_copy(c, (c + j) % cols).wait_send()


def solution(mesh):
    rows = mesh.shape['row']
    cols = mesh.shape['col']
    seq_spec = P(('dp', 'col', 'row'))
    act_spec = P('dp', ('row', 'col'))

    def local_layer(x, ln_gain, w_in, w_out, k_cache, v_cache, lengths, rope_cos, rope_sin):
        batch, xw = x.shape
        group = rows * cols
        seqs = batch // group
        head = rope_cos.shape[1] * 2
        cache_len = k_cache.shape[1]
        kdim, e_cols = w_in.shape
        r_cols, n_out = w_out.shape
        kv_cols = head // cols
        f_cols = e_cols - r_cols - 2 * kv_cols
        q_cols = r_cols - f_cols
        gate_start = q_cols + 2 * kv_cols
        heads = q_cols * cols // head
        w = CHUNK
        n_chunks = f_cols // 2 // w
        dims = (rows, cols, n_chunks, w, q_cols, kv_cols, f_cols)
        vmem = pl.BlockSpec(memory_space=pltpu.VMEM)
        hbm = pl.BlockSpec(memory_space=pl.ANY)
        dma = pltpu.SemaphoreType.DMA
        return pl.pallas_call(
            functools.partial(layer_kernel, dims),
            out_shape=(jax.ShapeDtypeStruct((batch, xw), BF16), pltpu.VMEM((seqs, cache_len, head), BF16),
                       pltpu.VMEM((seqs, cache_len, head), BF16)),
            in_specs=[pl.BlockSpec(memory_space=pltpu.SMEM), vmem, vmem, hbm, hbm, hbm, hbm, vmem, vmem],
            out_specs=(vmem, vmem, vmem),
            scratch_shapes=[
                pltpu.VMEM((kdim, gate_start), BF16),
                pltpu.VMEM((n_chunks, kdim, 4 * w), BF16),
                pltpu.VMEM((r_cols, n_out), BF16),
                pltpu.VMEM((cols, batch, xw), BF16),
                pltpu.VMEM((cols, 8, xw), F32),
                pltpu.VMEM((group, 8, batch), F32),
                pltpu.VMEM((batch, kdim), BF16),
                pltpu.VMEM((2, n_chunks, batch, 2 * w), BF16),
                pltpu.VMEM((2, n_chunks, batch, 2 * w), BF16),
                pltpu.VMEM((2, n_chunks, batch, w), BF16),
                pltpu.VMEM((group, seqs, gate_start), BF16),
                pltpu.VMEM((group, seqs, gate_start), BF16),
                pltpu.VMEM((heads, seqs, head), F32),
                pltpu.VMEM((seqs, heads, head), BF16),
                pltpu.VMEM((seqs, 8, head), F32),
                pltpu.VMEM((seqs, 8, head), F32),
                pltpu.VMEM((seqs, heads, head), F32),
                pltpu.VMEM((cols, seqs, q_cols), BF16),
                pltpu.VMEM((group, seqs, q_cols), BF16),
                pltpu.VMEM((batch, n_out), F32),
                pltpu.VMEM((cols, batch, xw), BF16),
                pltpu.VMEM((cols, batch, xw), BF16),
                dma((4 * n_chunks + 2,)), dma((2, seqs)),
                dma((cols,)), dma((cols,)), dma((cols,)), dma((cols,)),
                dma((group,)), dma((group,)), dma((group,)), dma((group,)),
                dma((2, n_chunks)), dma((2, n_chunks)), dma((2, n_chunks)), dma((2, n_chunks)),
                dma((group,)), dma((group,)), dma((cols,)), dma((cols,)),
            ],
            compiler_params=pltpu.CompilerParams(collective_id=0, has_side_effects=True,
                                                 vmem_limit_bytes=44 * 1024 * 1024),
            name="layer",
        )(lengths, x, ln_gain[None, :], w_in, w_out, k_cache, v_cache, rope_cos, rope_sin)

    return jax.shard_map(local_layer, mesh=mesh, in_specs=(act_spec, P(('row', 'col')), P('row', 'col'), P('col', 'row'), seq_spec, seq_spec, seq_spec, seq_spec, seq_spec), out_specs=(act_spec, seq_spec, seq_spec), check_vma=False)
```

```python
import contextlib
import functools

import jax
import jax.numpy as jnp
from jax import lax
from jax.experimental import pallas as pl
from jax.experimental.pallas import tpu as pltpu
from jax.sharding import PartitionSpec as P

NORM_EPS = 1e-6
MESH = pl.DeviceIdType.MESH
F32 = jnp.float32
BF16 = jnp.bfloat16
CHUNK = 128
FIRST = 4
BEFORE = 8
LAG = 3
ATTN_AT = 7
SEND_AT = 18
GATHER_AT = 15
GATHER_LAG = 3
PROFILE = False


def scope(name):
    return jax.named_scope(name) if PROFILE else contextlib.nullcontext()


def layer_kernel(dims, len_hbm, x_hbm, gain_hbm, win_ref, wout_ref, kc_ref, vc_ref, cos_hbm, sin_hbm,
                 y_refs, kbuf, vbuf,
                 len_ref, gain_ref, cos_ref, sin_ref, wq, wgu, wo, xg, gg, st, h, part, rbuf, mful, qsend, qrecv, qhm, qsm, kn3, vn3, osm,
                 asend, arecv, acc, total_ref,
                 isem, wsem, kvsem, xs_s, xs_r, g_s, g_r, st_s, st_r, q_s, q_r, rs_s, rs_r, ag_s, ag_r, at_s, at_r):
    rows, cols, n_chunks, w, q_cols, kv_cols, f_cols = dims
    group = rows * cols
    dp, r, c = lax.axis_index("dp"), lax.axis_index("row"), lax.axis_index("col")
    me = c * rows + r
    batch, xw = y_refs[0].shape
    seqs = batch // group
    gate_start = q_cols + 2 * kv_cols
    half_f = f_cols // 2
    heads_c = q_cols // 256
    heads = heads_c * cols
    cache_len, head = kbuf.shape[1:]

    def dev(g):
        return (dp, g % rows, g // rows)

    small = [pltpu.make_async_copy(src, dst, isem.at[i]) for i, (src, dst) in enumerate(
        ((x_hbm, xg.at[c]), (gain_hbm, gain_ref), (cos_hbm, cos_ref), (sin_hbm, sin_ref), (len_hbm, len_ref)))]
    for copy in small:
        copy.start()

    barrier = pltpu.get_barrier_semaphore()

    @pl.loop(1, group)
    def _(j):
        pl.semaphore_signal(barrier, inc=1, device_id=dev((me + j) % group), device_id_type=MESH)

    def wq_copy():
        return pltpu.make_async_copy(win_ref.at[:, pl.ds(0, gate_start)], wq, wsem.at[n_chunks])

    def wgu_copy(d, k, part_id):
        col = gate_start + part_id * f_cols + d * half_f + k * w
        return pltpu.make_async_copy(win_ref.at[:, pl.ds(pl.multiple_of(col, 128), w)],
                                     wgu.at[k, :, pl.ds((2 * d + part_id) * w, w)],
                                     wsem.at[k])

    def kv_copy(b, which):
        src, dst = ((kc_ref, kbuf), (vc_ref, vbuf))[which]
        return pltpu.make_async_copy(src.at[b], dst.at[b], kvsem.at[b])

    def wo_copy():
        return pltpu.make_async_copy(wout_ref, wo, wsem.at[n_chunks + 1])

    wq_copy().start()

    @pl.loop(0, n_chunks)
    def _(k):
        for d in range(2):
            for s in range(2):
                wgu_copy(d, k, s).start()

    @pl.loop(0, seqs)
    def _(b):
        kv_copy(b, 0).start()
        kv_copy(b, 1).start()

    wo_copy().start()

    def all_bytes(ref, n, send_sem, recv_sem):
        part_ref = ref.at[pl.ds(0, n)]
        return pltpu.make_async_remote_copy(part_ref, part_ref, send_sem, recv_sem,
                                            device_id=dev((me + 1) % group), device_id_type=MESH)

    small[0].wait()
    small[1].wait()
    x_own = xg[c].astype(F32)
    s_own = jnp.sum(x_own, axis=1, keepdims=True)
    m2_own = jnp.sum(jnp.square(x_own - s_own * (1.0 / xw)), axis=1, keepdims=True)
    lane = lax.broadcasted_iota(jnp.int32, (batch, 128), 1)
    table = jnp.where(lane == 0, s_own, jnp.where(lane == 1, m2_own, 0.0))
    st[me] = table.T[0:8, :]
    gg[c] = jnp.broadcast_to(gain_ref[...].astype(F32).reshape(1, xw), (8, xw))

    with scope('barrier'):
        pl.semaphore_wait(barrier, group - 1)

    def st_copy(slot, peer):
        return pltpu.make_async_remote_copy(st.at[slot], st.at[slot], st_s, st_r,
                                            device_id=dev(peer), device_id_type=MESH)

    def x_copy(slot, peer_c):
        return pltpu.make_async_remote_copy(xg.at[slot], xg.at[slot], xs_s, xs_r,
                                            device_id=(dp, r, peer_c), device_id_type=MESH)

    def g_copy(slot, peer_c):
        return pltpu.make_async_remote_copy(gg.at[slot], gg.at[slot], g_s, g_r,
                                            device_id=(dp, r, peer_c), device_id_type=MESH)

    @pl.loop(1, group)
    def _(j):
        st_copy(me, (me + j) % group).start()

    @pl.loop(1, cols)
    def _(j):
        x_copy(c, (c + j) % cols).start()
        g_copy(c, (c + j) % cols).start()


    with scope('stats'):
        all_bytes(st, group - 1, st_s, st_r).wait_recv()

    stats = st[...]
    sums = stats[:, 0:1, :]
    width = xw * group
    mean_row = jnp.sum(sums, axis=0) * (1.0 / width)
    dev_mean = sums * (1.0 / xw) - mean_row[None]
    m2_row = jnp.sum(stats[:, 1:2, :] + xw * jnp.square(dev_mean), axis=0)
    inv_row = lax.rsqrt(m2_row * (1.0 / width) + NORM_EPS)
    sub = lax.broadcasted_iota(jnp.int32, (128, batch), 0)
    back = jnp.where(sub == 0, mean_row, jnp.where(sub == 1, inv_row, 0.0)).T
    mean = back[:, 0:1]
    inv = back[:, 1:2]

    with scope('xwait'):
        all_bytes(xg, cols - 1, xs_s, xs_r).wait_recv()
        all_bytes(gg, cols - 1, g_s, g_r).wait_recv()

    for cc in range(cols):
        xv = xg[cc].astype(F32)
        gain = gg[cc, 0:1, :]
        h[:, cc * xw:(cc + 1) * xw] = ((xv - mean) * inv * gain).astype(BF16)

    acc[...] = jnp.zeros_like(acc)

    def rs_copy(d, k):
        nxt = (dp, r + 1, c) if d == 0 else (dp, r - 1, c)
        return pltpu.make_async_remote_copy(part.at[d, k], rbuf.at[d, k], rs_s.at[d], rs_r.at[d, k],
                                            device_id=nxt, device_id_type=MESH)

    def ag_copy(d, k):
        nxt = (dp, r - 1, c) if d == 0 else (dp, r + 1, c)
        return pltpu.make_async_remote_copy(mful.at[d, k], mful.at[d, k], ag_s.at[d], ag_r.at[d, k],
                                            device_id=nxt, device_id_type=MESH)

    pos = (r, rows - 1 - r)

    def partial_step(k):
        pltpu.make_async_copy(win_ref.at[:, pl.ds(0, 4 * w)], wgu.at[k], wsem.at[k]).wait()
        both = jnp.dot(h[...], wgu[k], preferred_element_type=F32).astype(BF16)
        for d in range(2):
            part[d, k] = both[:, d * 2 * w:(d + 1) * 2 * w]

            @pl.when(pos[d] == 0)
            def _():
                rs_copy(d, k).start()

    def out_step(d, k):
        row0 = pl.multiple_of(q_cols + d * half_f + k * w, 128)
        acc[...] += jnp.dot(mful[d, k], wo[pl.ds(row0, w), :], preferred_element_type=F32)

    def reduce_step(d, k):
        total = part[d, k].astype(F32) + rbuf[d, k].astype(F32)

        @pl.when(pos[d] < rows - 1)
        def _():
            part[d, k] = total.astype(BF16)
            rs_copy(d, k).start()

        @pl.when(pos[d] == rows - 1)
        def _():
            full = total.astype(BF16).astype(F32)
            gate, up = full[:, :w], full[:, w:]
            mful[d, k] = (jax.nn.silu(gate) * up).astype(BF16)
            ag_copy(d, k).start()
            out_step(d, k)

    def prepare_queries():
        all_bytes(qrecv, group - 1, q_s, q_r).wait_recv()

        cos_t, sin_t = cos_ref[...], sin_ref[...]

        def rope(v):
            first, second = v[:, :128], v[:, 128:]
            return jnp.concatenate([first * cos_t - second * sin_t, second * cos_t + first * sin_t], axis=-1)

        k_parts, v_parts = [], []
        for cc in range(cols):
            full = qrecv[cc * rows].astype(F32)
            for rr in range(1, rows):
                full = full + qrecv[cc * rows + rr].astype(F32)
            full = full.astype(BF16).astype(F32)
            for i in range(heads_c):
                qhm[cc * heads_c + i] = rope(full[:, i * 256:(i + 1) * 256]) * (256 ** -0.5)
            k_parts.append(full[:, q_cols:q_cols + kv_cols])
            v_parts.append(full[:, q_cols + kv_cols:gate_start])
        k_row = rope(jnp.concatenate(k_parts, axis=-1)).astype(BF16)
        v_row = jnp.concatenate(v_parts, axis=-1).astype(BF16)
        k_row, v_row = k_row.astype(F32), v_row.astype(F32)
        for b in range(seqs):
            qsm[b] = qhm[:, b, :].astype(BF16)
            kn3[b] = jnp.broadcast_to(k_row[b:b + 1, :], (8, 256))
            vn3[b] = jnp.broadcast_to(v_row[b:b + 1, :], (8, 256))

    def attend(b):
        pltpu.make_async_copy(kc_ref.at[pl.ds(0, 2)], kbuf.at[pl.ds(0, 2)], kvsem.at[b]).wait()
        limit = len_ref[b]
        slot = lax.broadcasted_iota(jnp.int32, (cache_len, head), 0) == limit
        k_all = jnp.where(slot, kn3[b][0:1, :].astype(BF16), kbuf[b])
        v_all = jnp.where(slot, vn3[b][0:1, :].astype(BF16), vbuf[b])
        kbuf[b] = k_all
        vbuf[b] = v_all
        scores = lax.dot_general(qsm[b], k_all, (((1,), (1,)), ((), ())), preferred_element_type=F32)
        where_t = lax.broadcasted_iota(jnp.int32, (heads, cache_len), 1)
        scores = jnp.where(where_t <= limit, scores, -1e30)
        e = jnp.exp(scores - jnp.max(scores, axis=1, keepdims=True))
        probs = (e / jnp.sum(e, axis=1, keepdims=True)).astype(BF16)
        osm[b] = jnp.dot(probs, v_all, preferred_element_type=F32)

    def at_copy(slot, peer):
        return pltpu.make_async_remote_copy(asend.at[peer // rows], arecv.at[slot], at_s, at_r,
                                            device_id=dev(peer), device_id_type=MESH)

    def send_attention():
        for cc in range(cols):
            asend[cc] = jnp.concatenate([osm[:, cc * heads_c + i, :] for i in range(heads_c)], axis=-1).astype(BF16)
        arecv[me] = asend[c]

        @pl.loop(1, group)
        def _(j):
            at_copy(me, (me + j) % group).start()

    @pl.loop(0, FIRST)
    def _(k):
        with scope('partial'):
            partial_step(k)

    def q_copy(slot, peer):
        return pltpu.make_async_remote_copy(qsend.at[peer], qrecv.at[slot], q_s, q_r,
                                            device_id=dev(peer), device_id_type=MESH)

    with scope('wqwait'):
        wq_copy().wait()
    qkv = jnp.dot(h[...], wq[...], preferred_element_type=F32)
    qsend[...] = qkv.reshape(group, seqs, gate_start).astype(BF16)
    qrecv[me] = qsend[me]

    @pl.loop(1, group)
    def _(j):
        q_copy(me, (me + j) % group).start()

    @pl.loop(FIRST, BEFORE)
    def _(k):
        with scope('partial'):
            partial_step(k)

    @pl.loop(0, max(GATHER_AT + GATHER_LAG * (rows - 2) + n_chunks // 2, LAG * (rows - 2) + n_chunks))
    def _(i):
        @pl.when(i == LAG)
        def _():
            wo_copy().wait()

        for half in range(2):
            @pl.when(BEFORE + 2 * i + half < n_chunks)
            def _():
                with scope('partial'):
                    partial_step(BEFORE + 2 * i + half)

        for d in range(2):
            p = pos[d]
            k = i - LAG * (p - 1)

            @pl.when((p > 0) & (k >= 0) & (k < n_chunks))
            def _():
                with scope('rswait%d' % d):
                    rs_copy(d, k).wait_recv()
                with scope('reduce%d' % d):
                    reduce_step(d, k)

        for d in range(2):
            q = rows - 1 - pos[d]
            k2 = i - GATHER_AT - GATHER_LAG * (q - 1)

            @pl.when((q > 0) & (k2 >= 0) & (k2 < n_chunks // 2))
            def _():
                for k in (2 * k2, 2 * k2 + 1):
                    with scope('agwait%d' % d):
                        ag_copy(d, k).wait_recv()

                    @pl.when(q < rows - 1)
                    def _():
                        ag_copy(d, k).start()

                    with scope('outstep'):
                        out_step(d, k)

        @pl.when(i == ATTN_AT - 1)
        def _():
            with scope('prepare'):
                for copy in small[2:]:
                    copy.wait()
                prepare_queries()

        @pl.when((i >= ATTN_AT) & (i < ATTN_AT + seqs))
        def _():
            with scope('attend'):
                attend(i - ATTN_AT)

        @pl.when(i == SEND_AT)
        def _():
            with scope('sendattn'):
                send_attention()

    with scope('atwait'):
        all_bytes(arecv, group - 1, at_s, at_r).wait_recv()

    with scope('final'):
        attn = arecv[...].astype(F32).reshape(batch, q_cols).astype(BF16)
        total = (acc[...] + jnp.dot(attn, wo[0:q_cols, :], preferred_element_type=F32)).astype(BF16)
        for cc in range(cols):
            total_ref[cc] = total[:, cc * xw:(cc + 1) * xw]
        for j in range(cols):
            y_refs[j][...] = total_ref[(c + j) % cols]

    all_bytes(st, group - 1, st_s, st_r).wait_send()
    all_bytes(qsend, group - 1, q_s, q_r).wait_send()
    all_bytes(arecv, group - 1, at_s, at_r).wait_send()
    all_bytes(xg, cols - 1, xs_s, xs_r).wait_send()
    all_bytes(gg, cols - 1, g_s, g_r).wait_send()
    for d in range(2):
        @pl.when(pos[d] < rows - 1)
        def _():
            all_bytes(part.at[d], n_chunks, rs_s.at[d], rs_s.at[d]).wait_send()

        @pl.when(pos[d] > 0)
        def _():
            all_bytes(mful.at[d], n_chunks, ag_s.at[d], ag_s.at[d]).wait_send()


def store_kernel(kbuf, vbuf, k_out, v_out, sem):
    copies = [pltpu.make_async_copy(src.at[b], dst.at[b], sem.at[i, b])
              for b in range(kbuf.shape[0]) for i, (src, dst) in enumerate(((kbuf, k_out), (vbuf, v_out)))]
    for copy in copies:
        copy.start()
    for copy in copies:
        copy.wait()


def solution(mesh):
    rows = mesh.shape['row']
    cols = mesh.shape['col']
    seq_spec = P(('dp', 'col', 'row'))
    act_spec = P('dp', ('row', 'col'))

    def local_layer(x, ln_gain, w_in, w_out, k_cache, v_cache, lengths, rope_cos, rope_sin):
        batch, xw = x.shape
        group = rows * cols
        seqs = batch // group
        head = rope_cos.shape[1] * 2
        cache_len = k_cache.shape[1]
        kdim, e_cols = w_in.shape
        r_cols, n_out = w_out.shape
        kv_cols = head // cols
        f_cols = e_cols - r_cols - 2 * kv_cols
        q_cols = r_cols - f_cols
        gate_start = q_cols + 2 * kv_cols
        heads = q_cols * cols // head
        w = CHUNK
        n_chunks = f_cols // 2 // w
        dims = (rows, cols, n_chunks, w, q_cols, kv_cols, f_cols)
        vmem = pl.BlockSpec(memory_space=pltpu.VMEM)
        hbm = pl.BlockSpec(memory_space=pl.ANY)
        dma = pltpu.SemaphoreType.DMA
        pieces, k_all, v_all = pl.pallas_call(
            functools.partial(layer_kernel, dims),
            out_shape=((jax.ShapeDtypeStruct((batch, xw), BF16),) * cols, pltpu.VMEM((seqs, cache_len, head), BF16),
                       pltpu.VMEM((seqs, cache_len, head), BF16)),
            in_specs=[hbm] * 9,
            out_specs=((vmem,) * cols, vmem, vmem),
            scratch_shapes=[
                pltpu.SMEM((seqs,), jnp.int32),
                pltpu.VMEM((xw,), BF16),
                pltpu.VMEM((seqs, head // 2), F32),
                pltpu.VMEM((seqs, head // 2), F32),
                pltpu.VMEM((kdim, gate_start), BF16),
                pltpu.VMEM((n_chunks, kdim, 4 * w), BF16),
                pltpu.VMEM((r_cols, n_out), BF16),
                pltpu.VMEM((cols, batch, xw), BF16),
                pltpu.VMEM((cols, 8, xw), F32),
                pltpu.VMEM((group, 8, batch), F32),
                pltpu.VMEM((batch, kdim), BF16),
                pltpu.VMEM((2, n_chunks, batch, 2 * w), BF16),
                pltpu.VMEM((2, n_chunks, batch, 2 * w), BF16),
                pltpu.VMEM((2, n_chunks, batch, w), BF16),
                pltpu.VMEM((group, seqs, gate_start), BF16),
                pltpu.VMEM((group, seqs, gate_start), BF16),
                pltpu.VMEM((heads, seqs, head), F32),
                pltpu.VMEM((seqs, heads, head), BF16),
                pltpu.VMEM((seqs, 8, head), F32),
                pltpu.VMEM((seqs, 8, head), F32),
                pltpu.VMEM((seqs, heads, head), F32),
                pltpu.VMEM((cols, seqs, q_cols), BF16),
                pltpu.VMEM((group, seqs, q_cols), BF16),
                pltpu.VMEM((batch, n_out), F32),
                pltpu.VMEM((cols, batch, xw), BF16),
                dma((5,)), dma((n_chunks + 2,)), dma((seqs,)),
                dma(()), dma(()), dma(()), dma(()), dma(()), dma(()), dma(()), dma(()),
                dma((2,)), dma((2, n_chunks)), dma((2,)), dma((2, n_chunks)),
                dma(()), dma(()),
            ],
            compiler_params=pltpu.CompilerParams(collective_id=0, has_side_effects=True,
                                                 vmem_limit_bytes=44 * 1024 * 1024),
            name="layer",
        )(lengths, x, ln_gain, w_in, w_out, k_cache, v_cache, rope_cos, rope_sin)
        delta = pieces[0].astype(F32)
        for j in range(1, cols):
            moved = lax.ppermute(pieces[j], 'col', [(s, (s + j) % cols) for s in range(cols)])
            delta = delta + moved.astype(F32)
        cache_bytes = 2 * k_all.size * 2
        k_out, v_out = pl.pallas_call(
            store_kernel,
            out_shape=(jax.ShapeDtypeStruct(k_all.shape, BF16),) * 2,
            in_specs=[vmem, vmem],
            out_specs=(hbm, hbm),
            scratch_shapes=[dma((2, seqs))],
            cost_estimate=pl.CostEstimate(flops=10 ** 8, bytes_accessed=cache_bytes, transcendentals=0),
            compiler_params=pltpu.CompilerParams(vmem_limit_bytes=1024 * 1024),
            name="store",
        )(k_all, v_all)
        y = (x.astype(F32) + delta.astype(BF16).astype(F32)).astype(BF16)
        return y, k_out, v_out

    return jax.shard_map(local_layer, mesh=mesh, in_specs=(act_spec, P(('row', 'col')), P('row', 'col'), P('col', 'row'), seq_spec, seq_spec, seq_spec, seq_spec, seq_spec), out_specs=(act_spec, seq_spec, seq_spec), check_vma=False)
```

```python
import contextlib
import functools

import jax
import jax.numpy as jnp
from jax import lax
from jax.experimental import pallas as pl
from jax.experimental.pallas import tpu as pltpu
from jax.sharding import PartitionSpec as P

NORM_EPS = 1e-6
MESH = pl.DeviceIdType.MESH
F32 = jnp.float32
BF16 = jnp.bfloat16
CHUNK = 128
FIRST = 4
BEFORE = 8
LAG = 3
ATTN_AT = 7
SEND_AT = 15
SPREAD = 3
GATHER_AT = 15
GATHER_LAG = 2
PROFILE = False


def scope(name):
    return jax.named_scope(name) if PROFILE else contextlib.nullcontext()


def layer_kernel(dims, len_hbm, x_hbm, gain_hbm, win_ref, wout_ref, kc_ref, vc_ref, cos_hbm, sin_hbm,
                 mine_ref, other_ref, kbuf, vbuf,
                 len_ref, gain_ref, cos_ref, sin_ref, wq, wgu, wo, xg, gg, st, h, part, rbuf, mful, qsend, qrecv, qhm, qsm, kn3, vn3, osm,
                 asend, arecv, acc, total_ref, pair,
                 isem, wsem, kvsem, xs_s, xs_r, g_s, g_r, st_s, st_r, q_s, q_r, rs_s, rs_r, ag_s, ag_r, ac_s, ac_r, ab_s, ab_r, pr_s, pr_r):
    rows, cols, n_chunks, w, q_cols, kv_cols, f_cols = dims
    group = rows * cols
    dp, r, c = lax.axis_index("dp"), lax.axis_index("row"), lax.axis_index("col")
    me = c * rows + r
    batch, xw = mine_ref.shape
    seqs = batch // group
    gate_start = q_cols + 2 * kv_cols
    half_f = f_cols // 2
    heads_c = q_cols // 256
    heads = heads_c * cols
    cache_len, head = kbuf.shape[1:]

    def dev(g):
        return (dp, g % rows, g // rows)

    small = [pltpu.make_async_copy(src, dst, isem.at[i]) for i, (src, dst) in enumerate(
        ((x_hbm, xg.at[c]), (gain_hbm, gain_ref), (cos_hbm, cos_ref), (sin_hbm, sin_ref), (len_hbm, len_ref)))]
    for copy in small:
        copy.start()

    barrier = pltpu.get_barrier_semaphore()

    @pl.loop(1, group)
    def _(j):
        pl.semaphore_signal(barrier, inc=1, device_id=dev((me + j) % group), device_id_type=MESH)

    def wq_copy():
        return pltpu.make_async_copy(win_ref.at[:, pl.ds(0, gate_start)], wq, wsem.at[n_chunks])

    def wgu_copy(d, k, part_id):
        col = gate_start + part_id * f_cols + d * half_f + k * w
        return pltpu.make_async_copy(win_ref.at[:, pl.ds(pl.multiple_of(col, 128), w)],
                                     wgu.at[k, :, pl.ds((2 * d + part_id) * w, w)],
                                     wsem.at[k])

    def kv_copy(b, which):
        src, dst = ((kc_ref, kbuf), (vc_ref, vbuf))[which]
        return pltpu.make_async_copy(src.at[b], dst.at[b], kvsem.at[b])

    def wo_copy():
        return pltpu.make_async_copy(wout_ref, wo, wsem.at[n_chunks + 1])

    wq_copy().start()

    @pl.loop(0, n_chunks)
    def _(k):
        for d in range(2):
            for s in range(2):
                wgu_copy(d, k, s).start()

    @pl.loop(0, seqs)
    def _(b):
        kv_copy(b, 0).start()
        kv_copy(b, 1).start()

    wo_copy().start()

    def all_bytes(ref, n, send_sem, recv_sem):
        part_ref = ref.at[pl.ds(0, n)]
        return pltpu.make_async_remote_copy(part_ref, part_ref, send_sem, recv_sem,
                                            device_id=dev((me + 1) % group), device_id_type=MESH)

    small[0].wait()
    small[1].wait()
    x_own = xg[c].astype(F32)
    s_own = jnp.sum(x_own, axis=1, keepdims=True)
    m2_own = jnp.sum(jnp.square(x_own - s_own * (1.0 / xw)), axis=1, keepdims=True)
    lane = lax.broadcasted_iota(jnp.int32, (batch, 128), 1)
    table = jnp.where(lane == 0, s_own, jnp.where(lane == 1, m2_own, 0.0))
    st[me] = table.T[0:8, :]
    gg[c] = jnp.broadcast_to(gain_ref[...].astype(F32).reshape(1, xw), (8, xw))

    with scope('barrier'):
        pl.semaphore_wait(barrier, group - 1)

    def st_copy(slot, peer):
        return pltpu.make_async_remote_copy(st.at[slot], st.at[slot], st_s, st_r,
                                            device_id=dev(peer), device_id_type=MESH)

    def x_copy(slot, peer_c):
        return pltpu.make_async_remote_copy(xg.at[slot], xg.at[slot], xs_s, xs_r,
                                            device_id=(dp, r, peer_c), device_id_type=MESH)

    def g_copy(slot, peer_c):
        return pltpu.make_async_remote_copy(gg.at[slot], gg.at[slot], g_s, g_r,
                                            device_id=(dp, r, peer_c), device_id_type=MESH)

    @pl.loop(1, group)
    def _(j):
        st_copy(me, (me + j) % group).start()

    @pl.loop(1, cols)
    def _(j):
        x_copy(c, (c + j) % cols).start()
        g_copy(c, (c + j) % cols).start()


    with scope('stats'):
        all_bytes(st, group - 1, st_s, st_r).wait_recv()

    stats = st[...]
    sums = stats[:, 0:1, :]
    width = xw * group
    mean_row = jnp.sum(sums, axis=0) * (1.0 / width)
    dev_mean = sums * (1.0 / xw) - mean_row[None]
    m2_row = jnp.sum(stats[:, 1:2, :] + xw * jnp.square(dev_mean), axis=0)
    inv_row = lax.rsqrt(m2_row * (1.0 / width) + NORM_EPS)
    sub = lax.broadcasted_iota(jnp.int32, (128, batch), 0)
    back = jnp.where(sub == 0, mean_row, jnp.where(sub == 1, inv_row, 0.0)).T
    mean = back[:, 0:1]
    inv = back[:, 1:2]

    with scope('xwait'):
        all_bytes(xg, cols - 1, xs_s, xs_r).wait_recv()
        all_bytes(gg, cols - 1, g_s, g_r).wait_recv()

    for cc in range(cols):
        xv = xg[cc].astype(F32)
        gain = gg[cc, 0:1, :]
        h[:, cc * xw:(cc + 1) * xw] = ((xv - mean) * inv * gain).astype(BF16)

    acc[...] = jnp.zeros_like(acc)

    def rs_copy(d, k):
        nxt = (dp, r + 1, c) if d == 0 else (dp, r - 1, c)
        return pltpu.make_async_remote_copy(part.at[d, k], rbuf.at[d, k], rs_s.at[d], rs_r.at[d, k],
                                            device_id=nxt, device_id_type=MESH)

    def ag_copy(d, k):
        nxt = (dp, r - 1, c) if d == 0 else (dp, r + 1, c)
        return pltpu.make_async_remote_copy(mful.at[d, k], mful.at[d, k], ag_s.at[d], ag_r.at[d, k],
                                            device_id=nxt, device_id_type=MESH)

    pos = (r, rows - 1 - r)

    def partial_step(k):
        pltpu.make_async_copy(win_ref.at[:, pl.ds(0, 4 * w)], wgu.at[k], wsem.at[k]).wait()
        both = jnp.dot(h[...], wgu[k], preferred_element_type=F32).astype(BF16)
        for d in range(2):
            part[d, k] = both[:, d * 2 * w:(d + 1) * 2 * w]

            @pl.when(pos[d] == 0)
            def _():
                rs_copy(d, k).start()

    def out_step(d, k):
        row0 = pl.multiple_of(q_cols + d * half_f + k * w, 128)
        acc[...] += jnp.dot(mful[d, k], wo[pl.ds(row0, w), :], preferred_element_type=F32)

    def reduce_step(d, k):
        total = part[d, k].astype(F32) + rbuf[d, k].astype(F32)

        @pl.when(pos[d] < rows - 1)
        def _():
            part[d, k] = total.astype(BF16)
            rs_copy(d, k).start()

        @pl.when(pos[d] == rows - 1)
        def _():
            full = total.astype(BF16).astype(F32)
            gate, up = full[:, :w], full[:, w:]
            mful[d, k] = (jax.nn.silu(gate) * up).astype(BF16)
            ag_copy(d, k).start()
            out_step(d, k)

    def prepare_queries():
        all_bytes(qrecv, group - 1, q_s, q_r).wait_recv()

        cos_t, sin_t = cos_ref[...], sin_ref[...]

        def rope(v):
            first, second = v[:, :128], v[:, 128:]
            return jnp.concatenate([first * cos_t - second * sin_t, second * cos_t + first * sin_t], axis=-1)

        k_parts, v_parts = [], []
        for cc in range(cols):
            full = qrecv[cc * rows].astype(F32)
            for rr in range(1, rows):
                full = full + qrecv[cc * rows + rr].astype(F32)
            full = full.astype(BF16).astype(F32)
            for i in range(heads_c):
                qhm[cc * heads_c + i] = rope(full[:, i * 256:(i + 1) * 256]) * (256 ** -0.5)
            k_parts.append(full[:, q_cols:q_cols + kv_cols])
            v_parts.append(full[:, q_cols + kv_cols:gate_start])
        k_row = rope(jnp.concatenate(k_parts, axis=-1)).astype(BF16)
        v_row = jnp.concatenate(v_parts, axis=-1).astype(BF16)
        k_row, v_row = k_row.astype(F32), v_row.astype(F32)
        for b in range(seqs):
            qsm[b] = qhm[:, b, :].astype(BF16)
            kn3[b] = jnp.broadcast_to(k_row[b:b + 1, :], (8, 256))
            vn3[b] = jnp.broadcast_to(v_row[b:b + 1, :], (8, 256))

    def attend(b):
        pltpu.make_async_copy(kc_ref.at[pl.ds(0, 2)], kbuf.at[pl.ds(0, 2)], kvsem.at[b]).wait()
        limit = len_ref[b]
        slot = lax.broadcasted_iota(jnp.int32, (cache_len, head), 0) == limit
        k_all = jnp.where(slot, kn3[b][0:1, :].astype(BF16), kbuf[b])
        v_all = jnp.where(slot, vn3[b][0:1, :].astype(BF16), vbuf[b])
        kbuf[b] = k_all
        vbuf[b] = v_all
        scores = lax.dot_general(qsm[b], k_all, (((1,), (1,)), ((), ())), preferred_element_type=F32)
        where_t = lax.broadcasted_iota(jnp.int32, (heads, cache_len), 1)
        scores = jnp.where(where_t <= limit, scores, -1e30)
        e = jnp.exp(scores - jnp.max(scores, axis=1, keepdims=True))
        probs = (e / jnp.sum(e, axis=1, keepdims=True)).astype(BF16)
        osm[b] = jnp.dot(probs, v_all, preferred_element_type=F32)

    def ac_copy(peer_c):
        return pltpu.make_async_remote_copy(asend.at[peer_c], arecv.at[r, c], ac_s, ac_r,
                                            device_id=(dp, r, peer_c), device_id_type=MESH)

    def ab_copy(d, rr):
        return pltpu.make_async_remote_copy(arecv.at[rr], arecv.at[rr], ab_s.at[d, rr], ab_r.at[d, rr],
                                            device_id=(dp, r + 1 - 2 * d, c), device_id_type=MESH)

    def send_attention():
        for cc in range(cols):
            asend[cc] = jnp.concatenate([osm[:, cc * heads_c + i, :] for i in range(heads_c)], axis=-1).astype(BF16)
        arecv[r, c] = asend[c]

        @pl.loop(1, cols)
        def _(j):
            ac_copy((c + j) % cols).start()

    def spread_attention(t):
        if t == 0:
            all_bytes(arecv.at[r], cols - 1, ac_s, ac_r).wait_recv()
        for d in range(2):
            rr = r - t + 2 * t * d

            @pl.when(t <= pos[d])
            def _():
                if t > 0:
                    ab_copy(d, rr).wait_recv()

                @pl.when(pos[d] < rows - 1)
                def _():
                    ab_copy(d, rr).start()

    @pl.loop(0, FIRST)
    def _(k):
        with scope('partial'):
            partial_step(k)

    def q_copy(slot, peer):
        return pltpu.make_async_remote_copy(qsend.at[peer], qrecv.at[slot], q_s, q_r,
                                            device_id=dev(peer), device_id_type=MESH)

    with scope('wqwait'):
        wq_copy().wait()
    qkv = jnp.dot(h[...], wq[...], preferred_element_type=F32)
    qsend[...] = qkv.reshape(group, seqs, gate_start).astype(BF16)
    qrecv[me] = qsend[me]

    @pl.loop(1, group)
    def _(j):
        q_copy(me, (me + j) % group).start()

    @pl.loop(FIRST, BEFORE)
    def _(k):
        with scope('partial'):
            partial_step(k)

    @pl.loop(0, max(GATHER_AT + GATHER_LAG * (rows - 2) + n_chunks // 2, SEND_AT + SPREAD * rows + 1, LAG * (rows - 2) + n_chunks))
    def _(i):
        @pl.when(i == LAG)
        def _():
            wo_copy().wait()

        for half in range(2):
            @pl.when(BEFORE + 2 * i + half < n_chunks)
            def _():
                with scope('partial'):
                    partial_step(BEFORE + 2 * i + half)

        for d in range(2):
            p = pos[d]
            k = i - LAG * (p - 1)

            @pl.when((p > 0) & (k >= 0) & (k < n_chunks))
            def _():
                with scope('rswait%d' % d):
                    rs_copy(d, k).wait_recv()
                with scope('reduce%d' % d):
                    reduce_step(d, k)

        for d in range(2):
            q = rows - 1 - pos[d]
            k2 = i - GATHER_AT - GATHER_LAG * (q - 1)

            @pl.when((q > 0) & (k2 >= 0) & (k2 < n_chunks // 2))
            def _():
                for k in (2 * k2, 2 * k2 + 1):
                    with scope('agwait%d' % d):
                        ag_copy(d, k).wait_recv()

                    @pl.when(q < rows - 1)
                    def _():
                        ag_copy(d, k).start()

                    with scope('outstep'):
                        out_step(d, k)

        @pl.when(i == ATTN_AT - 1)
        def _():
            with scope('prepare'):
                for copy in small[2:]:
                    copy.wait()
                prepare_queries()

        @pl.when((i >= ATTN_AT) & (i < ATTN_AT + seqs))
        def _():
            with scope('attend'):
                attend(i - ATTN_AT)

        @pl.when(i == SEND_AT)
        def _():
            with scope('sendattn'):
                send_attention()

        for t in range(rows):
            @pl.when(i == SEND_AT + SPREAD * (t + 1))
            def _():
                with scope('spread%d' % t):
                    spread_attention(t)

    with scope('final'):
        attn = jnp.concatenate([arecv[rr, cc].astype(F32) for cc in range(cols) for rr in range(rows)], axis=0).astype(BF16)
        total = (acc[...] + jnp.dot(attn, wo[0:q_cols, :], preferred_element_type=F32)).astype(BF16)
        for cc in range(cols):
            total_ref[cc] = total[:, cc * xw:(cc + 1) * xw]

    mate = c + 1 - 2 * (c % 2)
    across = (c + 2) % cols

    def pair_copy(i):
        return pltpu.make_async_remote_copy(total_ref.at[(mate + 2 * i) % cols], pair.at[i], pr_s, pr_r,
                                            device_id=(dp, r, mate), device_id_type=MESH)

    pair_copy(1).start()
    pair_copy(0).start()

    all_bytes(st, group - 1, st_s, st_r).wait_send()
    all_bytes(qsend, group - 1, q_s, q_r).wait_send()
    all_bytes(asend, cols - 1, ac_s, ac_r).wait_send()
    all_bytes(xg, cols - 1, xs_s, xs_r).wait_send()
    all_bytes(gg, cols - 1, g_s, g_r).wait_send()
    for d in range(2):
        @pl.when(pos[d] < rows - 1)
        def _():
            all_bytes(part.at[d], n_chunks, rs_s.at[d], rs_s.at[d]).wait_send()

            for t in range(rows):
                @pl.when(t <= pos[d])
                def _():
                    ab_copy(d, r - t + 2 * t * d).wait_send()

        @pl.when(pos[d] > 0)
        def _():
            all_bytes(mful.at[d], n_chunks, ag_s.at[d], ag_s.at[d]).wait_send()

    with scope('pair'):
        all_bytes(pair, 2, pr_s, pr_r).wait_recv()
    other_ref[...] = (total_ref[across].astype(F32) + pair[1].astype(F32)).astype(BF16)
    mine_ref[...] = total_ref[c].astype(F32) + pair[0].astype(F32)
    all_bytes(pair, 2, pr_s, pr_r).wait_send()


def store_kernel(kbuf, vbuf, k_out, v_out, sem):
    copies = [pltpu.make_async_copy(src.at[b], dst.at[b], sem.at[i, b])
              for b in range(kbuf.shape[0]) for i, (src, dst) in enumerate(((kbuf, k_out), (vbuf, v_out)))]
    for copy in copies:
        copy.start()
    for copy in copies:
        copy.wait()


def solution(mesh):
    rows = mesh.shape['row']
    cols = mesh.shape['col']
    seq_spec = P(('dp', 'col', 'row'))
    act_spec = P('dp', ('row', 'col'))

    def local_layer(x, ln_gain, w_in, w_out, k_cache, v_cache, lengths, rope_cos, rope_sin):
        batch, xw = x.shape
        group = rows * cols
        seqs = batch // group
        head = rope_cos.shape[1] * 2
        cache_len = k_cache.shape[1]
        kdim, e_cols = w_in.shape
        r_cols, n_out = w_out.shape
        kv_cols = head // cols
        f_cols = e_cols - r_cols - 2 * kv_cols
        q_cols = r_cols - f_cols
        gate_start = q_cols + 2 * kv_cols
        heads = q_cols * cols // head
        w = CHUNK
        n_chunks = f_cols // 2 // w
        dims = (rows, cols, n_chunks, w, q_cols, kv_cols, f_cols)
        vmem = pl.BlockSpec(memory_space=pltpu.VMEM)
        hbm = pl.BlockSpec(memory_space=pl.ANY)
        dma = pltpu.SemaphoreType.DMA
        mine, other, k_all, v_all = pl.pallas_call(
            functools.partial(layer_kernel, dims),
            out_shape=(pltpu.VMEM((batch, xw), F32), pltpu.VMEM((batch, xw), BF16), pltpu.VMEM((seqs, cache_len, head), BF16),
                       pltpu.VMEM((seqs, cache_len, head), BF16)),
            in_specs=[hbm] * 9,
            out_specs=(vmem, vmem, vmem, vmem),
            scratch_shapes=[
                pltpu.SMEM((seqs,), jnp.int32),
                pltpu.VMEM((xw,), BF16),
                pltpu.VMEM((seqs, head // 2), F32),
                pltpu.VMEM((seqs, head // 2), F32),
                pltpu.VMEM((kdim, gate_start), BF16),
                pltpu.VMEM((n_chunks, kdim, 4 * w), BF16),
                pltpu.VMEM((r_cols, n_out), BF16),
                pltpu.VMEM((cols, batch, xw), BF16),
                pltpu.VMEM((cols, 8, xw), F32),
                pltpu.VMEM((group, 8, batch), F32),
                pltpu.VMEM((batch, kdim), BF16),
                pltpu.VMEM((2, n_chunks, batch, 2 * w), BF16),
                pltpu.VMEM((2, n_chunks, batch, 2 * w), BF16),
                pltpu.VMEM((2, n_chunks, batch, w), BF16),
                pltpu.VMEM((group, seqs, gate_start), BF16),
                pltpu.VMEM((group, seqs, gate_start), BF16),
                pltpu.VMEM((heads, seqs, head), F32),
                pltpu.VMEM((seqs, heads, head), BF16),
                pltpu.VMEM((seqs, 8, head), F32),
                pltpu.VMEM((seqs, 8, head), F32),
                pltpu.VMEM((seqs, heads, head), F32),
                pltpu.VMEM((cols, seqs, q_cols), BF16),
                pltpu.VMEM((rows, cols, seqs, q_cols), BF16),
                pltpu.VMEM((batch, n_out), F32),
                pltpu.VMEM((cols, batch, xw), BF16),
                pltpu.VMEM((2, batch, xw), BF16),
                dma((5,)), dma((n_chunks + 2,)), dma((seqs,)),
                dma(()), dma(()), dma(()), dma(()), dma(()), dma(()), dma(()), dma(()),
                dma((2,)), dma((2, n_chunks)), dma((2,)), dma((2, n_chunks)),
                dma(()), dma(()), dma((2, rows)), dma((2, rows)), dma(()), dma(()),
            ],
            compiler_params=pltpu.CompilerParams(collective_id=0, has_side_effects=True,
                                                 vmem_limit_bytes=44 * 1024 * 1024),
            name="layer",
        )(lengths, x, ln_gain, w_in, w_out, k_cache, v_cache, rope_cos, rope_sin)
        moved = lax.ppermute(other, 'col', [(s, (s + 2) % cols) for s in range(cols)])
        delta = mine + moved.astype(F32)
        cache_bytes = 2 * k_all.size * 2
        k_out, v_out = pl.pallas_call(
            store_kernel,
            out_shape=(jax.ShapeDtypeStruct(k_all.shape, BF16),) * 2,
            in_specs=[vmem, vmem],
            out_specs=(hbm, hbm),
            scratch_shapes=[dma((2, seqs))],
            cost_estimate=pl.CostEstimate(flops=10 ** 8, bytes_accessed=cache_bytes, transcendentals=0),
            compiler_params=pltpu.CompilerParams(vmem_limit_bytes=1024 * 1024),
            name="store",
        )(k_all, v_all)
        y = (x.astype(F32) + delta.astype(BF16).astype(F32)).astype(BF16)
        return y, k_out, v_out

    return jax.shard_map(local_layer, mesh=mesh, in_specs=(act_spec, P(('row', 'col')), P('row', 'col'), P('col', 'row'), seq_spec, seq_spec, seq_spec, seq_spec, seq_spec), out_specs=(act_spec, seq_spec, seq_spec), check_vma=False)
```

```python
import contextlib
import functools

import jax
import jax.numpy as jnp
from jax import lax
from jax.experimental import pallas as pl
from jax.experimental.pallas import tpu as pltpu
from jax.sharding import PartitionSpec as P

NORM_EPS = 1e-6
MESH = pl.DeviceIdType.MESH
F32 = jnp.float32
BF16 = jnp.bfloat16
CHUNK = 128
FIRST = 4
BEFORE = 8
LAG = 2
ATTN_AT = 7
SEND_AT = 15
SPREAD = 2
GATHER_AT = 15
GATHER_LAG = 2
PROFILE = False


def scope(name):
    return jax.named_scope(name) if PROFILE else contextlib.nullcontext()


def layer_kernel(dims, len_hbm, x_hbm, gain_hbm, win_ref, wout_ref, kc_ref, vc_ref, cos_hbm, sin_hbm,
                 mine_ref, other_ref, kbuf, vbuf,
                 len_ref, gain_ref, cos_ref, sin_ref, wq, wgu, wo, xg, gg, st, h, part, rbuf, mful, qsend, qrecv, qhm, qsm, kn3, vn3, osm,
                 asend, arecv, acc, total_ref, pair,
                 isem, wsem, kvsem, xs_s, xs_r, g_s, g_r, st_s, st_r, q_s, q_r, rs_s, rs_r, ag_s, ag_r, ac_s, ac_r, ab_s, ab_r, pr_s, pr_r):
    rows, cols, n_chunks, w, q_cols, kv_cols, f_cols = dims
    group = rows * cols
    dp, r, c = lax.axis_index("dp"), lax.axis_index("row"), lax.axis_index("col")
    me = c * rows + r
    batch, xw = mine_ref.shape
    seqs = batch // group
    gate_start = q_cols + 2 * kv_cols
    half_f = f_cols // 2
    heads_c = q_cols // 256
    heads = heads_c * cols
    cache_len, head = kbuf.shape[1:]

    def dev(g):
        return (dp, g % rows, g // rows)

    small = [pltpu.make_async_copy(src, dst, isem.at[i]) for i, (src, dst) in enumerate(
        ((x_hbm, xg.at[c]), (gain_hbm, gain_ref), (cos_hbm, cos_ref), (sin_hbm, sin_ref), (len_hbm, len_ref)))]
    for copy in small:
        copy.start()

    barrier = pltpu.get_barrier_semaphore()

    @pl.loop(1, group)
    def _(j):
        pl.semaphore_signal(barrier, inc=1, device_id=dev((me + j) % group), device_id_type=MESH)

    def wq_copy():
        return pltpu.make_async_copy(win_ref.at[:, pl.ds(0, gate_start)], wq, wsem.at[n_chunks])

    def wgu_copy(d, k, part_id):
        col = gate_start + part_id * f_cols + d * half_f + k * w
        return pltpu.make_async_copy(win_ref.at[:, pl.ds(pl.multiple_of(col, 128), w)],
                                     wgu.at[k, :, pl.ds((2 * d + part_id) * w, w)],
                                     wsem.at[k])

    def kv_copy(b, which):
        src, dst = ((kc_ref, kbuf), (vc_ref, vbuf))[which]
        return pltpu.make_async_copy(src.at[b], dst.at[b], kvsem.at[b])

    def wo_copy():
        return pltpu.make_async_copy(wout_ref, wo, wsem.at[n_chunks + 1])

    wq_copy().start()

    @pl.loop(0, n_chunks)
    def _(k):
        for d in range(2):
            for s in range(2):
                wgu_copy(d, k, s).start()

    @pl.loop(0, seqs)
    def _(b):
        kv_copy(b, 0).start()
        kv_copy(b, 1).start()

    wo_copy().start()

    def all_bytes(ref, n, send_sem, recv_sem):
        part_ref = ref.at[pl.ds(0, n)]
        return pltpu.make_async_remote_copy(part_ref, part_ref, send_sem, recv_sem,
                                            device_id=dev((me + 1) % group), device_id_type=MESH)

    small[0].wait()
    small[1].wait()
    x_own = xg[c].astype(F32)
    s_own = jnp.sum(x_own, axis=1, keepdims=True)
    m2_own = jnp.sum(jnp.square(x_own - s_own * (1.0 / xw)), axis=1, keepdims=True)
    lane = lax.broadcasted_iota(jnp.int32, (batch, 128), 1)
    table = jnp.where(lane == 0, s_own, jnp.where(lane == 1, m2_own, 0.0))
    st[me] = table.T[0:8, :]
    gg[c] = jnp.broadcast_to(gain_ref[...].astype(F32).reshape(1, xw), (8, xw))

    with scope('barrier'):
        pl.semaphore_wait(barrier, group - 1)

    def st_copy(slot, peer):
        return pltpu.make_async_remote_copy(st.at[slot], st.at[slot], st_s, st_r,
                                            device_id=dev(peer), device_id_type=MESH)

    def x_copy(slot, peer_c):
        return pltpu.make_async_remote_copy(xg.at[slot], xg.at[slot], xs_s, xs_r,
                                            device_id=(dp, r, peer_c), device_id_type=MESH)

    def g_copy(slot, peer_c):
        return pltpu.make_async_remote_copy(gg.at[slot], gg.at[slot], g_s, g_r,
                                            device_id=(dp, r, peer_c), device_id_type=MESH)

    @pl.loop(1, group)
    def _(j):
        st_copy(me, (me + j) % group).start()

    @pl.loop(1, cols)
    def _(j):
        x_copy(c, (c + j) % cols).start()
        g_copy(c, (c + j) % cols).start()


    with scope('stats'):
        all_bytes(st, group - 1, st_s, st_r).wait_recv()

    stats = st[...]
    sums = stats[:, 0:1, :]
    width = xw * group
    mean_row = jnp.sum(sums, axis=0) * (1.0 / width)
    dev_mean = sums * (1.0 / xw) - mean_row[None]
    m2_row = jnp.sum(stats[:, 1:2, :] + xw * jnp.square(dev_mean), axis=0)
    inv_row = lax.rsqrt(m2_row * (1.0 / width) + NORM_EPS)
    sub = lax.broadcasted_iota(jnp.int32, (128, batch), 0)
    back = jnp.where(sub == 0, mean_row, jnp.where(sub == 1, inv_row, 0.0)).T
    mean = back[:, 0:1]
    inv = back[:, 1:2]

    with scope('xwait'):
        all_bytes(xg, cols - 1, xs_s, xs_r).wait_recv()
        all_bytes(gg, cols - 1, g_s, g_r).wait_recv()

    for cc in range(cols):
        xv = xg[cc].astype(F32)
        gain = gg[cc, 0:1, :]
        h[:, cc * xw:(cc + 1) * xw] = ((xv - mean) * inv * gain).astype(BF16)

    acc[...] = jnp.zeros_like(acc)

    def rs_copy(d, k):
        nxt = (dp, r + 1, c) if d == 0 else (dp, r - 1, c)
        return pltpu.make_async_remote_copy(part.at[d, k], rbuf.at[d, k], rs_s.at[d], rs_r.at[d, k],
                                            device_id=nxt, device_id_type=MESH)

    def ag_copy(d, k):
        nxt = (dp, r - 1, c) if d == 0 else (dp, r + 1, c)
        return pltpu.make_async_remote_copy(mful.at[d, k], mful.at[d, k], ag_s.at[d], ag_r.at[d, k],
                                            device_id=nxt, device_id_type=MESH)

    pos = (r, rows - 1 - r)

    def partial_step(k):
        pltpu.make_async_copy(win_ref.at[:, pl.ds(0, 4 * w)], wgu.at[k], wsem.at[k]).wait()
        both = jnp.dot(h[...], wgu[k], preferred_element_type=F32).astype(BF16)
        for d in range(2):
            part[d, k] = both[:, d * 2 * w:(d + 1) * 2 * w]

            @pl.when(pos[d] == 0)
            def _():
                rs_copy(d, k).start()

    def out_step(d, k):
        row0 = pl.multiple_of(q_cols + d * half_f + k * w, 128)
        acc[...] += jnp.dot(mful[d, k], wo[pl.ds(row0, w), :], preferred_element_type=F32)

    def reduce_step(d, k):
        total = part[d, k].astype(F32) + rbuf[d, k].astype(F32)

        @pl.when(pos[d] < rows - 1)
        def _():
            part[d, k] = total.astype(BF16)
            rs_copy(d, k).start()

        @pl.when(pos[d] == rows - 1)
        def _():
            full = total.astype(BF16).astype(F32)
            gate, up = full[:, :w], full[:, w:]
            mful[d, k] = (jax.nn.silu(gate) * up).astype(BF16)
            ag_copy(d, k).start()
            out_step(d, k)

    def prepare_queries():
        all_bytes(qrecv, group - 1, q_s, q_r).wait_recv()

        cos_t, sin_t = cos_ref[...], sin_ref[...]

        def rope(v):
            first, second = v[:, :128], v[:, 128:]
            return jnp.concatenate([first * cos_t - second * sin_t, second * cos_t + first * sin_t], axis=-1)

        k_parts, v_parts = [], []
        for cc in range(cols):
            full = qrecv[cc * rows].astype(F32)
            for rr in range(1, rows):
                full = full + qrecv[cc * rows + rr].astype(F32)
            full = full.astype(BF16).astype(F32)
            for i in range(heads_c):
                qhm[cc * heads_c + i] = rope(full[:, i * 256:(i + 1) * 256]) * (256 ** -0.5)
            k_parts.append(full[:, q_cols:q_cols + kv_cols])
            v_parts.append(full[:, q_cols + kv_cols:gate_start])
        k_row = rope(jnp.concatenate(k_parts, axis=-1)).astype(BF16)
        v_row = jnp.concatenate(v_parts, axis=-1).astype(BF16)
        k_row, v_row = k_row.astype(F32), v_row.astype(F32)
        for b in range(seqs):
            qsm[b] = qhm[:, b, :].astype(BF16)
            kn3[b] = jnp.broadcast_to(k_row[b:b + 1, :], (8, 256))
            vn3[b] = jnp.broadcast_to(v_row[b:b + 1, :], (8, 256))

    def attend(b):
        pltpu.make_async_copy(kc_ref.at[pl.ds(0, 2)], kbuf.at[pl.ds(0, 2)], kvsem.at[b]).wait()
        limit = len_ref[b]
        slot = lax.broadcasted_iota(jnp.int32, (cache_len, head), 0) == limit
        k_all = jnp.where(slot, kn3[b][0:1, :].astype(BF16), kbuf[b])
        v_all = jnp.where(slot, vn3[b][0:1, :].astype(BF16), vbuf[b])
        kbuf[b] = k_all
        vbuf[b] = v_all
        scores = lax.dot_general(qsm[b], k_all, (((1,), (1,)), ((), ())), preferred_element_type=F32)
        where_t = lax.broadcasted_iota(jnp.int32, (heads, cache_len), 1)
        scores = jnp.where(where_t <= limit, scores, -1e30)
        e = jnp.exp(scores - jnp.max(scores, axis=1, keepdims=True))
        probs = (e / jnp.sum(e, axis=1, keepdims=True)).astype(BF16)
        osm[b] = jnp.dot(probs, v_all, preferred_element_type=F32)

    def ac_copy(peer_c):
        return pltpu.make_async_remote_copy(asend.at[peer_c], arecv.at[r, c], ac_s, ac_r,
                                            device_id=(dp, r, peer_c), device_id_type=MESH)

    def ab_copy(d, rr):
        return pltpu.make_async_remote_copy(arecv.at[rr], arecv.at[rr], ab_s.at[d, rr], ab_r.at[d, rr],
                                            device_id=(dp, r + 1 - 2 * d, c), device_id_type=MESH)

    def send_attention():
        for cc in range(cols):
            asend[cc] = jnp.concatenate([osm[:, cc * heads_c + i, :] for i in range(heads_c)], axis=-1).astype(BF16)
        arecv[r, c] = asend[c]

        @pl.loop(1, cols)
        def _(j):
            ac_copy((c + j) % cols).start()

    def spread_attention(t):
        if t == 0:
            all_bytes(arecv.at[r], cols - 1, ac_s, ac_r).wait_recv()
        for d in range(2):
            rr = r - t + 2 * t * d

            @pl.when(t <= pos[d])
            def _():
                if t > 0:
                    ab_copy(d, rr).wait_recv()

                @pl.when(pos[d] < rows - 1)
                def _():
                    ab_copy(d, rr).start()

    @pl.loop(0, FIRST)
    def _(k):
        with scope('partial'):
            partial_step(k)

    def q_copy(slot, peer):
        return pltpu.make_async_remote_copy(qsend.at[peer], qrecv.at[slot], q_s, q_r,
                                            device_id=dev(peer), device_id_type=MESH)

    with scope('wqwait'):
        wq_copy().wait()
    qkv = jnp.dot(h[...], wq[...], preferred_element_type=F32)
    qsend[...] = qkv.reshape(group, seqs, gate_start).astype(BF16)
    qrecv[me] = qsend[me]

    @pl.loop(1, group)
    def _(j):
        q_copy(me, (me + j) % group).start()

    @pl.loop(FIRST, BEFORE)
    def _(k):
        with scope('partial'):
            partial_step(k)

    @pl.loop(0, max(GATHER_AT + GATHER_LAG * (rows - 2) + n_chunks // 2, SEND_AT + SPREAD * rows + 1, LAG * (rows - 2) + n_chunks))
    def _(i):
        @pl.when(i == LAG)
        def _():
            wo_copy().wait()

        for half in range(2):
            @pl.when(BEFORE + 2 * i + half < n_chunks)
            def _():
                with scope('partial'):
                    partial_step(BEFORE + 2 * i + half)

        for d in range(2):
            @pl.when((pos[d] == 1) & (i < n_chunks))
            def _():
                with scope('rswait%d' % d):
                    rs_copy(d, i).wait_recv()
                part[d, i] = (part[d, i].astype(F32) + rbuf[d, i].astype(F32)).astype(BF16)
                rs_copy(d, i).start()

        @pl.when((i >= ATTN_AT) & (i < ATTN_AT + seqs))
        def _():
            with scope('attend'):
                attend(i - ATTN_AT)

        for d in range(2):
            p = pos[d]
            k = i - LAG * (p - 1)

            @pl.when((p > 1) & (k >= 0) & (k < n_chunks))
            def _():
                with scope('rswait%d' % d):
                    rs_copy(d, k).wait_recv()
                with scope('reduce%d' % d):
                    reduce_step(d, k)

        for d in range(2):
            q = rows - 1 - pos[d]
            k2 = i - GATHER_AT - GATHER_LAG * (q - 1)

            @pl.when((q > 0) & (k2 >= 0) & (k2 < n_chunks // 2))
            def _():
                for k in (2 * k2, 2 * k2 + 1):
                    with scope('agwait%d' % d):
                        ag_copy(d, k).wait_recv()

                    @pl.when(q < rows - 1)
                    def _():
                        ag_copy(d, k).start()

                    with scope('outstep'):
                        out_step(d, k)

        @pl.when(i == ATTN_AT - 1)
        def _():
            with scope('prepare'):
                for copy in small[2:]:
                    copy.wait()
                prepare_queries()

        @pl.when(i == SEND_AT)
        def _():
            with scope('sendattn'):
                send_attention()

        for t in range(rows):
            @pl.when(i == SEND_AT + SPREAD * (t + 1))
            def _():
                with scope('spread%d' % t):
                    spread_attention(t)
                    if t == rows - 1:
                        attn = jnp.concatenate([arecv[rr, cc].astype(F32) for cc in range(cols) for rr in range(rows)], axis=0)
                        acc[...] += jnp.dot(attn.astype(BF16), wo[0:q_cols, :], preferred_element_type=F32)

    with scope('final'):
        total = acc[...].astype(BF16)
        for cc in range(cols):
            total_ref[cc] = total[:, cc * xw:(cc + 1) * xw]

    mate = c + 1 - 2 * (c % 2)
    across = (c + 2) % cols

    def pair_copy(i):
        return pltpu.make_async_remote_copy(total_ref.at[(mate + 2 * i) % cols], pair.at[i], pr_s, pr_r,
                                            device_id=(dp, r, mate), device_id_type=MESH)

    pair_copy(1).start()
    pair_copy(0).start()

    all_bytes(st, group - 1, st_s, st_r).wait_send()
    all_bytes(qsend, group - 1, q_s, q_r).wait_send()
    all_bytes(asend, cols - 1, ac_s, ac_r).wait_send()
    all_bytes(xg, cols - 1, xs_s, xs_r).wait_send()
    all_bytes(gg, cols - 1, g_s, g_r).wait_send()
    for d in range(2):
        @pl.when(pos[d] < rows - 1)
        def _():
            all_bytes(part.at[d], n_chunks, rs_s.at[d], rs_s.at[d]).wait_send()

            for t in range(rows):
                @pl.when(t <= pos[d])
                def _():
                    ab_copy(d, r - t + 2 * t * d).wait_send()

        @pl.when(pos[d] > 0)
        def _():
            all_bytes(mful.at[d], n_chunks, ag_s.at[d], ag_s.at[d]).wait_send()

    with scope('pair'):
        all_bytes(pair, 2, pr_s, pr_r).wait_recv()
    other_ref[...] = (total_ref[across].astype(F32) + pair[1].astype(F32)).astype(BF16)
    mine_ref[...] = total_ref[c].astype(F32) + pair[0].astype(F32)
    all_bytes(pair, 2, pr_s, pr_r).wait_send()


def store_kernel(kbuf, vbuf, k_out, v_out, sem):
    copies = [pltpu.make_async_copy(src.at[b], dst.at[b], sem.at[i, b])
              for b in range(kbuf.shape[0]) for i, (src, dst) in enumerate(((kbuf, k_out), (vbuf, v_out)))]
    for copy in copies:
        copy.start()
    for copy in copies:
        copy.wait()


def solution(mesh):
    rows = mesh.shape['row']
    cols = mesh.shape['col']
    seq_spec = P(('dp', 'col', 'row'))
    act_spec = P('dp', ('row', 'col'))

    def local_layer(x, ln_gain, w_in, w_out, k_cache, v_cache, lengths, rope_cos, rope_sin):
        batch, xw = x.shape
        group = rows * cols
        seqs = batch // group
        head = rope_cos.shape[1] * 2
        cache_len = k_cache.shape[1]
        kdim, e_cols = w_in.shape
        r_cols, n_out = w_out.shape
        kv_cols = head // cols
        f_cols = e_cols - r_cols - 2 * kv_cols
        q_cols = r_cols - f_cols
        gate_start = q_cols + 2 * kv_cols
        heads = q_cols * cols // head
        w = CHUNK
        n_chunks = f_cols // 2 // w
        dims = (rows, cols, n_chunks, w, q_cols, kv_cols, f_cols)
        vmem = pl.BlockSpec(memory_space=pltpu.VMEM)
        hbm = pl.BlockSpec(memory_space=pl.ANY)
        dma = pltpu.SemaphoreType.DMA
        mine, other, k_all, v_all = pl.pallas_call(
            functools.partial(layer_kernel, dims),
            out_shape=(pltpu.VMEM((batch, xw), F32), pltpu.VMEM((batch, xw), BF16), pltpu.VMEM((seqs, cache_len, head), BF16),
                       pltpu.VMEM((seqs, cache_len, head), BF16)),
            in_specs=[hbm] * 9,
            out_specs=(vmem, vmem, vmem, vmem),
            scratch_shapes=[
                pltpu.SMEM((seqs,), jnp.int32),
                pltpu.VMEM((xw,), BF16),
                pltpu.VMEM((seqs, head // 2), F32),
                pltpu.VMEM((seqs, head // 2), F32),
                pltpu.VMEM((kdim, gate_start), BF16),
                pltpu.VMEM((n_chunks, kdim, 4 * w), BF16),
                pltpu.VMEM((r_cols, n_out), BF16),
                pltpu.VMEM((cols, batch, xw), BF16),
                pltpu.VMEM((cols, 8, xw), F32),
                pltpu.VMEM((group, 8, batch), F32),
                pltpu.VMEM((batch, kdim), BF16),
                pltpu.VMEM((2, n_chunks, batch, 2 * w), BF16),
                pltpu.VMEM((2, n_chunks, batch, 2 * w), BF16),
                pltpu.VMEM((2, n_chunks, batch, w), BF16),
                pltpu.VMEM((group, seqs, gate_start), BF16),
                pltpu.VMEM((group, seqs, gate_start), BF16),
                pltpu.VMEM((heads, seqs, head), F32),
                pltpu.VMEM((seqs, heads, head), BF16),
                pltpu.VMEM((seqs, 8, head), F32),
                pltpu.VMEM((seqs, 8, head), F32),
                pltpu.VMEM((seqs, heads, head), F32),
                pltpu.VMEM((cols, seqs, q_cols), BF16),
                pltpu.VMEM((rows, cols, seqs, q_cols), BF16),
                pltpu.VMEM((batch, n_out), F32),
                pltpu.VMEM((cols, batch, xw), BF16),
                pltpu.VMEM((2, batch, xw), BF16),
                dma((5,)), dma((n_chunks + 2,)), dma((seqs,)),
                dma(()), dma(()), dma(()), dma(()), dma(()), dma(()), dma(()), dma(()),
                dma((2,)), dma((2, n_chunks)), dma((2,)), dma((2, n_chunks)),
                dma(()), dma(()), dma((2, rows)), dma((2, rows)), dma(()), dma(()),
            ],
            compiler_params=pltpu.CompilerParams(collective_id=0, has_side_effects=True,
                                                 vmem_limit_bytes=44 * 1024 * 1024),
            name="layer",
        )(lengths, x, ln_gain, w_in, w_out, k_cache, v_cache, rope_cos, rope_sin)
        moved = lax.ppermute(other, 'col', [(s, (s + 2) % cols) for s in range(cols)])
        delta = mine + moved.astype(F32)
        cache_bytes = 2 * k_all.size * 2
        k_out, v_out = pl.pallas_call(
            store_kernel,
            out_shape=(jax.ShapeDtypeStruct(k_all.shape, BF16),) * 2,
            in_specs=[vmem, vmem],
            out_specs=(hbm, hbm),
            scratch_shapes=[dma((2, seqs))],
            cost_estimate=pl.CostEstimate(flops=10 ** 8, bytes_accessed=cache_bytes, transcendentals=0),
            compiler_params=pltpu.CompilerParams(vmem_limit_bytes=1024 * 1024),
            name="store",
        )(k_all, v_all)
        y = (x.astype(F32) + delta.astype(BF16).astype(F32)).astype(BF16)
        return y, k_out, v_out

    return jax.shard_map(local_layer, mesh=mesh, in_specs=(act_spec, P(('row', 'col')), P('row', 'col'), P('col', 'row'), seq_spec, seq_spec, seq_spec, seq_spec, seq_spec), out_specs=(act_spec, seq_spec, seq_spec), check_vma=False)
```

```python
import contextlib
import functools

import jax
import jax.numpy as jnp
from jax import lax
from jax.experimental import pallas as pl
from jax.experimental.pallas import tpu as pltpu
from jax.sharding import PartitionSpec as P

NORM_EPS = 1e-6
MESH = pl.DeviceIdType.MESH
F32 = jnp.float32
BF16 = jnp.bfloat16
CHUNK = 128
FIRST = 4
BEFORE = 8
LAG = 2
ATTN_AT = 7
SEND_AT = 15
SPREAD = 2
GATHER_AT = 15
GATHER_LAG = 2
PROFILE = False


def scope(name):
    return jax.named_scope(name) if PROFILE else contextlib.nullcontext()


def layer_kernel(dims, len_hbm, x_hbm, gain_hbm, win_ref, wout_ref, kc_ref, vc_ref, cos_hbm, sin_hbm,
                 mine_ref, other_ref, kbuf, vbuf,
                 len_ref, gain_ref, cos_ref, sin_ref, wq, wgu, wo, xg, gg, st, h, part, rbuf, mful, qsend, qrecv, qhm, qsm, kn3, vn3, osm,
                 asend, arecv, acc, total_ref, pair,
                 isem, wsem, kvsem, xs_s, xs_r, g_s, g_r, st_s, st_r, q_s, q_r, rs_s, rs_r, ag_s, ag_r, ac_s, ac_r, ab_s, ab_r, pr_s, pr_r):
    rows, cols, n_chunks, w, q_cols, kv_cols, f_cols = dims
    group = rows * cols
    dp, r, c = lax.axis_index("dp"), lax.axis_index("row"), lax.axis_index("col")
    me = c * rows + r
    batch, xw = mine_ref.shape
    seqs = batch // group
    gate_start = q_cols + 2 * kv_cols
    half_f = f_cols // 2
    heads_c = q_cols // 256
    heads = heads_c * cols
    cache_len, head = kbuf.shape[1:]

    def dev(g):
        return (dp, g % rows, g // rows)

    small = [pltpu.make_async_copy(src, dst, isem.at[i]) for i, (src, dst) in enumerate(
        ((x_hbm, xg.at[c]), (gain_hbm, gain_ref), (cos_hbm, cos_ref), (sin_hbm, sin_ref), (len_hbm, len_ref)))]
    for copy in small:
        copy.start()

    barrier = pltpu.get_barrier_semaphore()

    @pl.loop(1, group)
    def _(j):
        pl.semaphore_signal(barrier, inc=1, device_id=dev((me + j) % group), device_id_type=MESH)

    def wq_copy():
        return pltpu.make_async_copy(win_ref.at[:, pl.ds(0, gate_start)], wq, wsem.at[n_chunks])

    def wgu_copy(d, k, part_id):
        col = gate_start + part_id * f_cols + d * half_f + k * w
        return pltpu.make_async_copy(win_ref.at[:, pl.ds(pl.multiple_of(col, 128), w)],
                                     wgu.at[k, :, pl.ds((2 * d + part_id) * w, w)],
                                     wsem.at[k])

    def kv_copy(b, which):
        src, dst = ((kc_ref, kbuf), (vc_ref, vbuf))[which]
        return pltpu.make_async_copy(src.at[b], dst.at[b], kvsem.at[b])

    def wo_copy():
        return pltpu.make_async_copy(wout_ref, wo, wsem.at[n_chunks + 1])

    wq_copy().start()

    @pl.loop(0, n_chunks)
    def _(k):
        for d in range(2):
            for s in range(2):
                wgu_copy(d, k, s).start()

    @pl.loop(0, seqs)
    def _(b):
        kv_copy(b, 0).start()
        kv_copy(b, 1).start()

    wo_copy().start()

    def all_bytes(ref, n, send_sem, recv_sem):
        part_ref = ref.at[pl.ds(0, n)]
        return pltpu.make_async_remote_copy(part_ref, part_ref, send_sem, recv_sem,
                                            device_id=dev((me + 1) % group), device_id_type=MESH)

    small[0].wait()
    small[1].wait()
    x_own = xg[c].astype(F32)
    s_own = jnp.sum(x_own, axis=1, keepdims=True)
    m2_own = jnp.sum(jnp.square(x_own - s_own * (1.0 / xw)), axis=1, keepdims=True)
    lane = lax.broadcasted_iota(jnp.int32, (batch, 128), 1)
    table = jnp.where(lane == 0, s_own, jnp.where(lane == 1, m2_own, 0.0))
    st[me] = table.T[0:8, :]
    gg[c] = jnp.broadcast_to(gain_ref[...].astype(F32).reshape(1, xw), (8, xw))

    with scope('barrier'):
        pl.semaphore_wait(barrier, group - 1)

    def st_copy(slot, peer):
        return pltpu.make_async_remote_copy(st.at[slot], st.at[slot], st_s, st_r,
                                            device_id=dev(peer), device_id_type=MESH)

    def x_copy(slot, peer_c):
        return pltpu.make_async_remote_copy(xg.at[slot], xg.at[slot], xs_s, xs_r,
                                            device_id=(dp, r, peer_c), device_id_type=MESH)

    def g_copy(slot, peer_c):
        return pltpu.make_async_remote_copy(gg.at[slot], gg.at[slot], g_s, g_r,
                                            device_id=(dp, r, peer_c), device_id_type=MESH)

    @pl.loop(1, cols)
    def _(j):
        g_copy(c, (c + j) % cols).start()
        x_copy(c, (c + j) % cols).start()

    @pl.loop(1, group)
    def _(j):
        st_copy(me, (me + j) % group).start()


    with scope('stats'):
        all_bytes(st, group - 1, st_s, st_r).wait_recv()

    stats = st[...]
    sums = stats[:, 0:1, :]
    width = xw * group
    mean_row = jnp.sum(sums, axis=0) * (1.0 / width)
    dev_mean = sums * (1.0 / xw) - mean_row[None]
    m2_row = jnp.sum(stats[:, 1:2, :] + xw * jnp.square(dev_mean), axis=0)
    inv_row = lax.rsqrt(m2_row * (1.0 / width) + NORM_EPS)
    sub = lax.broadcasted_iota(jnp.int32, (128, batch), 0)
    back = jnp.where(sub == 0, mean_row, jnp.where(sub == 1, inv_row, 0.0)).T
    mean = back[:, 0:1]
    inv = back[:, 1:2]

    with scope('xwait'):
        all_bytes(xg, cols - 1, xs_s, xs_r).wait_recv()
        all_bytes(gg, cols - 1, g_s, g_r).wait_recv()

    for cc in range(cols):
        xv = xg[cc].astype(F32)
        gain = gg[cc, 0:1, :]
        h[:, cc * xw:(cc + 1) * xw] = ((xv - mean) * inv * gain).astype(BF16)

    acc[...] = jnp.zeros_like(acc)

    def rs_copy(d, k):
        nxt = (dp, r + 1, c) if d == 0 else (dp, r - 1, c)
        return pltpu.make_async_remote_copy(part.at[d, k], rbuf.at[d, k], rs_s.at[d], rs_r.at[d, k],
                                            device_id=nxt, device_id_type=MESH)

    def ag_copy(d, k):
        nxt = (dp, r - 1, c) if d == 0 else (dp, r + 1, c)
        return pltpu.make_async_remote_copy(mful.at[d, k], mful.at[d, k], ag_s.at[d], ag_r.at[d, k],
                                            device_id=nxt, device_id_type=MESH)

    pos = (r, rows - 1 - r)

    def partial_step(k):
        pltpu.make_async_copy(win_ref.at[:, pl.ds(0, 4 * w)], wgu.at[k], wsem.at[k]).wait()
        both = jnp.dot(h[...], wgu[k], preferred_element_type=F32).astype(BF16)
        for d in range(2):
            part[d, k] = both[:, d * 2 * w:(d + 1) * 2 * w]

            @pl.when(pos[d] == 0)
            def _():
                rs_copy(d, k).start()

    def out_step(d, k):
        row0 = pl.multiple_of(q_cols + d * half_f + k * w, 128)
        acc[...] += jnp.dot(mful[d, k], wo[pl.ds(row0, w), :], preferred_element_type=F32)

    def reduce_step(d, k):
        total = part[d, k].astype(F32) + rbuf[d, k].astype(F32)

        @pl.when(pos[d] < rows - 1)
        def _():
            part[d, k] = total.astype(BF16)
            rs_copy(d, k).start()

        @pl.when(pos[d] == rows - 1)
        def _():
            full = total.astype(BF16).astype(F32)
            gate, up = full[:, :w], full[:, w:]
            mful[d, k] = (jax.nn.silu(gate) * up).astype(BF16)
            ag_copy(d, k).start()
            out_step(d, k)

    def prepare_queries():
        all_bytes(qrecv, group - 1, q_s, q_r).wait_recv()

        cos_t, sin_t = cos_ref[...], sin_ref[...]

        def rope(v):
            first, second = v[:, :128], v[:, 128:]
            return jnp.concatenate([first * cos_t - second * sin_t, second * cos_t + first * sin_t], axis=-1)

        k_parts, v_parts = [], []
        for cc in range(cols):
            full = qrecv[cc * rows].astype(F32)
            for rr in range(1, rows):
                full = full + qrecv[cc * rows + rr].astype(F32)
            full = full.astype(BF16).astype(F32)
            for i in range(heads_c):
                qhm[cc * heads_c + i] = rope(full[:, i * 256:(i + 1) * 256]) * (256 ** -0.5)
            k_parts.append(full[:, q_cols:q_cols + kv_cols])
            v_parts.append(full[:, q_cols + kv_cols:gate_start])
        k_row = rope(jnp.concatenate(k_parts, axis=-1)).astype(BF16)
        v_row = jnp.concatenate(v_parts, axis=-1).astype(BF16)
        k_row, v_row = k_row.astype(F32), v_row.astype(F32)
        for b in range(seqs):
            qsm[b] = qhm[:, b, :].astype(BF16)
            kn3[b] = jnp.broadcast_to(k_row[b:b + 1, :], (8, 256))
            vn3[b] = jnp.broadcast_to(v_row[b:b + 1, :], (8, 256))

    def attend(b):
        pltpu.make_async_copy(kc_ref.at[pl.ds(0, 2)], kbuf.at[pl.ds(0, 2)], kvsem.at[b]).wait()
        limit = len_ref[b]
        slot = lax.broadcasted_iota(jnp.int32, (cache_len, head), 0) == limit
        k_all = jnp.where(slot, kn3[b][0:1, :].astype(BF16), kbuf[b])
        v_all = jnp.where(slot, vn3[b][0:1, :].astype(BF16), vbuf[b])
        kbuf[b] = k_all
        vbuf[b] = v_all
        scores = lax.dot_general(qsm[b], k_all, (((1,), (1,)), ((), ())), preferred_element_type=F32)
        where_t = lax.broadcasted_iota(jnp.int32, (heads, cache_len), 1)
        scores = jnp.where(where_t <= limit, scores, -1e30)
        e = jnp.exp(scores - jnp.max(scores, axis=1, keepdims=True))
        probs = (e / jnp.sum(e, axis=1, keepdims=True)).astype(BF16)
        osm[b] = jnp.dot(probs, v_all, preferred_element_type=F32)

    def ac_copy(peer_c):
        return pltpu.make_async_remote_copy(asend.at[peer_c], arecv.at[r, c], ac_s, ac_r,
                                            device_id=(dp, r, peer_c), device_id_type=MESH)

    def ab_copy(d, rr):
        return pltpu.make_async_remote_copy(arecv.at[rr], arecv.at[rr], ab_s.at[d, rr], ab_r.at[d, rr],
                                            device_id=(dp, r + 1 - 2 * d, c), device_id_type=MESH)

    def send_attention():
        for cc in range(cols):
            asend[cc] = jnp.concatenate([osm[:, cc * heads_c + i, :] for i in range(heads_c)], axis=-1).astype(BF16)
        arecv[r, c] = asend[c]

        @pl.loop(1, cols)
        def _(j):
            ac_copy((c + j) % cols).start()

    def spread_attention(t):
        if t == 0:
            all_bytes(arecv.at[r], cols - 1, ac_s, ac_r).wait_recv()
        for d in range(2):
            rr = r - t + 2 * t * d

            @pl.when(t <= pos[d])
            def _():
                if t > 0:
                    ab_copy(d, rr).wait_recv()

                @pl.when(pos[d] < rows - 1)
                def _():
                    ab_copy(d, rr).start()

    @pl.loop(0, FIRST)
    def _(k):
        with scope('partial'):
            partial_step(k)

    def q_copy(slot, peer):
        return pltpu.make_async_remote_copy(qsend.at[peer], qrecv.at[slot], q_s, q_r,
                                            device_id=dev(peer), device_id_type=MESH)

    with scope('wqwait'):
        wq_copy().wait()
    qkv = jnp.dot(h[...], wq[...], preferred_element_type=F32)
    qsend[...] = qkv.reshape(group, seqs, gate_start).astype(BF16)
    qrecv[me] = qsend[me]

    @pl.loop(1, group)
    def _(j):
        q_copy(me, (me + j) % group).start()

    @pl.loop(FIRST, BEFORE)
    def _(k):
        with scope('partial'):
            partial_step(k)

    @pl.loop(0, max(GATHER_AT + GATHER_LAG * (rows - 2) + n_chunks // 2, SEND_AT + SPREAD * rows + 1, LAG * (rows - 2) + n_chunks))
    def _(i):
        @pl.when(i == LAG)
        def _():
            wo_copy().wait()

        for half in range(2):
            @pl.when(BEFORE + 2 * i + half < n_chunks)
            def _():
                with scope('partial'):
                    partial_step(BEFORE + 2 * i + half)

        for d in range(2):
            @pl.when((pos[d] == 1) & (i < n_chunks))
            def _():
                with scope('rswait%d' % d):
                    rs_copy(d, i).wait_recv()
                part[d, i] = (part[d, i].astype(F32) + rbuf[d, i].astype(F32)).astype(BF16)
                rs_copy(d, i).start()

        @pl.when((i >= ATTN_AT) & (i < ATTN_AT + seqs))
        def _():
            with scope('attend'):
                attend(i - ATTN_AT)

        for d in range(2):
            p = pos[d]
            k = i - LAG * (p - 1)

            @pl.when((p > 1) & (k >= 0) & (k < n_chunks))
            def _():
                with scope('rswait%d' % d):
                    rs_copy(d, k).wait_recv()
                with scope('reduce%d' % d):
                    reduce_step(d, k)

        for d in range(2):
            q = rows - 1 - pos[d]
            k2 = i - GATHER_AT - GATHER_LAG * (q - 1)

            @pl.when((q > 0) & (k2 >= 0) & (k2 < n_chunks // 2))
            def _():
                for k in (2 * k2, 2 * k2 + 1):
                    with scope('agwait%d' % d):
                        ag_copy(d, k).wait_recv()

                    @pl.when(q < rows - 1)
                    def _():
                        ag_copy(d, k).start()

                    with scope('outstep'):
                        out_step(d, k)

        @pl.when(i == ATTN_AT - 1)
        def _():
            with scope('prepare'):
                for copy in small[2:]:
                    copy.wait()
                prepare_queries()

        @pl.when(i == SEND_AT)
        def _():
            with scope('sendattn'):
                send_attention()

        for t in range(rows):
            @pl.when(i == SEND_AT + SPREAD * (t + 1))
            def _():
                with scope('spread%d' % t):
                    spread_attention(t)
                    if t == rows - 1:
                        attn = jnp.concatenate([arecv[rr, cc].astype(F32) for cc in range(cols) for rr in range(rows)], axis=0)
                        acc[...] += jnp.dot(attn.astype(BF16), wo[0:q_cols, :], preferred_element_type=F32)

    with scope('final'):
        total = acc[...].astype(BF16)
        for cc in range(cols):
            total_ref[cc] = total[:, cc * xw:(cc + 1) * xw]

    mate = c + 1 - 2 * (c % 2)
    across = (c + 2) % cols

    def pair_copy(i):
        return pltpu.make_async_remote_copy(total_ref.at[(mate + 2 * i) % cols], pair.at[i], pr_s, pr_r,
                                            device_id=(dp, r, mate), device_id_type=MESH)

    pair_copy(1).start()
    pair_copy(0).start()

    all_bytes(st, group - 1, st_s, st_r).wait_send()
    all_bytes(qsend, group - 1, q_s, q_r).wait_send()
    all_bytes(asend, cols - 1, ac_s, ac_r).wait_send()
    all_bytes(xg, cols - 1, xs_s, xs_r).wait_send()
    all_bytes(gg, cols - 1, g_s, g_r).wait_send()
    for d in range(2):
        @pl.when(pos[d] < rows - 1)
        def _():
            all_bytes(part.at[d], n_chunks, rs_s.at[d], rs_s.at[d]).wait_send()

            for t in range(rows):
                @pl.when(t <= pos[d])
                def _():
                    ab_copy(d, r - t + 2 * t * d).wait_send()

        @pl.when(pos[d] > 0)
        def _():
            all_bytes(mful.at[d], n_chunks, ag_s.at[d], ag_s.at[d]).wait_send()

    with scope('pair'):
        all_bytes(pair, 2, pr_s, pr_r).wait_recv()
    other_ref[...] = (total_ref[across].astype(F32) + pair[1].astype(F32)).astype(BF16)
    mine_ref[...] = total_ref[c].astype(F32) + pair[0].astype(F32)
    all_bytes(pair, 2, pr_s, pr_r).wait_send()


def store_kernel(kbuf, vbuf, k_out, v_out, sem):
    copies = [pltpu.make_async_copy(src.at[b], dst.at[b], sem.at[i, b])
              for b in range(kbuf.shape[0]) for i, (src, dst) in enumerate(((kbuf, k_out), (vbuf, v_out)))]
    for copy in copies:
        copy.start()
    for copy in copies:
        copy.wait()


def solution(mesh):
    rows = mesh.shape['row']
    cols = mesh.shape['col']
    seq_spec = P(('dp', 'col', 'row'))
    act_spec = P('dp', ('row', 'col'))

    def local_layer(x, ln_gain, w_in, w_out, k_cache, v_cache, lengths, rope_cos, rope_sin):
        batch, xw = x.shape
        group = rows * cols
        seqs = batch // group
        head = rope_cos.shape[1] * 2
        cache_len = k_cache.shape[1]
        kdim, e_cols = w_in.shape
        r_cols, n_out = w_out.shape
        kv_cols = head // cols
        f_cols = e_cols - r_cols - 2 * kv_cols
        q_cols = r_cols - f_cols
        gate_start = q_cols + 2 * kv_cols
        heads = q_cols * cols // head
        w = CHUNK
        n_chunks = f_cols // 2 // w
        dims = (rows, cols, n_chunks, w, q_cols, kv_cols, f_cols)
        vmem = pl.BlockSpec(memory_space=pltpu.VMEM)
        hbm = pl.BlockSpec(memory_space=pl.ANY)
        dma = pltpu.SemaphoreType.DMA
        mine, other, k_all, v_all = pl.pallas_call(
            functools.partial(layer_kernel, dims),
            out_shape=(pltpu.VMEM((batch, xw), F32), pltpu.VMEM((batch, xw), BF16), pltpu.VMEM((seqs, cache_len, head), BF16),
                       pltpu.VMEM((seqs, cache_len, head), BF16)),
            in_specs=[hbm] * 9,
            out_specs=(vmem, vmem, vmem, vmem),
            scratch_shapes=[
                pltpu.SMEM((seqs,), jnp.int32),
                pltpu.VMEM((xw,), BF16),
                pltpu.VMEM((seqs, head // 2), F32),
                pltpu.VMEM((seqs, head // 2), F32),
                pltpu.VMEM((kdim, gate_start), BF16),
                pltpu.VMEM((n_chunks, kdim, 4 * w), BF16),
                pltpu.VMEM((r_cols, n_out), BF16),
                pltpu.VMEM((cols, batch, xw), BF16),
                pltpu.VMEM((cols, 8, xw), F32),
                pltpu.VMEM((group, 8, batch), F32),
                pltpu.VMEM((batch, kdim), BF16),
                pltpu.VMEM((2, n_chunks, batch, 2 * w), BF16),
                pltpu.VMEM((2, n_chunks, batch, 2 * w), BF16),
                pltpu.VMEM((2, n_chunks, batch, w), BF16),
                pltpu.VMEM((group, seqs, gate_start), BF16),
                pltpu.VMEM((group, seqs, gate_start), BF16),
                pltpu.VMEM((heads, seqs, head), F32),
                pltpu.VMEM((seqs, heads, head), BF16),
                pltpu.VMEM((seqs, 8, head), F32),
                pltpu.VMEM((seqs, 8, head), F32),
                pltpu.VMEM((seqs, heads, head), F32),
                pltpu.VMEM((cols, seqs, q_cols), BF16),
                pltpu.VMEM((rows, cols, seqs, q_cols), BF16),
                pltpu.VMEM((batch, n_out), F32),
                pltpu.VMEM((cols, batch, xw), BF16),
                pltpu.VMEM((2, batch, xw), BF16),
                dma((5,)), dma((n_chunks + 2,)), dma((seqs,)),
                dma(()), dma(()), dma(()), dma(()), dma(()), dma(()), dma(()), dma(()),
                dma((2,)), dma((2, n_chunks)), dma((2,)), dma((2, n_chunks)),
                dma(()), dma(()), dma((2, rows)), dma((2, rows)), dma(()), dma(()),
            ],
            compiler_params=pltpu.CompilerParams(collective_id=0, has_side_effects=True,
                                                 vmem_limit_bytes=44 * 1024 * 1024),
            name="layer",
        )(lengths, x, ln_gain, w_in, w_out, k_cache, v_cache, rope_cos, rope_sin)
        moved = lax.ppermute(other, 'col', [(s, (s + 2) % cols) for s in range(cols)])
        delta = mine + moved.astype(F32)
        cache_bytes = 2 * k_all.size * 2
        k_out, v_out = pl.pallas_call(
            store_kernel,
            out_shape=(jax.ShapeDtypeStruct(k_all.shape, BF16),) * 2,
            in_specs=[vmem, vmem],
            out_specs=(hbm, hbm),
            scratch_shapes=[dma((2, seqs))],
            cost_estimate=pl.CostEstimate(flops=10 ** 8, bytes_accessed=cache_bytes, transcendentals=0),
            compiler_params=pltpu.CompilerParams(vmem_limit_bytes=1024 * 1024),
            name="store",
        )(k_all, v_all)
        y = (x.astype(F32) + delta.astype(BF16).astype(F32)).astype(BF16)
        return y, k_out, v_out

    return jax.shard_map(local_layer, mesh=mesh, in_specs=(act_spec, P(('row', 'col')), P('row', 'col'), P('col', 'row'), seq_spec, seq_spec, seq_spec, seq_spec, seq_spec), out_specs=(act_spec, seq_spec, seq_spec), check_vma=False)
```
